128 devices in a mesh: row: 8 (over y, core), col: 16 (over x, z).
Axes of the slice: x: 4, y: 4, z: 4, core: 2. Of those that a mesh axis runs over, the one named last changes fastest.
Arguments:
- observed: bfloat16 [128, 512, 188], P('row', 'col'), may hold values from -6 to 6
- library: bfloat16 [188, 2048], replicated, may hold values from -0.125 to 0.125
- warm: bfloat16 [128, 512, 2048], P('row', 'col'), may hold values from 0 to 1
- match_peer: int32 [32, 16, 8], P('row', 'col'), may hold values from 0 to 15
- match_slot: int32 [32, 16, 8], P('row', 'col'), may hold values from 0 to 1
- match_count: int32 [32, 16], P('row', 'col'), may hold values from 1 to 8
- match_weight: float32 [32, 16, 8], P('row', 'col'), may hold values from 0.1 to 10
- wanted: int32 [8, 256, 2], P('row', 'col'), may hold values from 0 to 3
- threshold: float32 [2048], replicated, may hold values from 0.02 to 0.2
Outputs:
- abundance: bfloat16 [128, 512, 2048], P('row', 'col')
- misfit: float32 [128, 512, 188], P('row', 'col')
The draws below stay inside these ranges and needn't reach their ends.
Inputs may be any that keep to these rules, and one draw needn't show every extreme that they name: `match_peer`: col index along the device's own col group. `wanted`: every device names exactly 2 blocks, repeats allowed, of every device of its col group, itself included.
All inputs are finite; a program needn't handle non-finite values.
Results may differ from the reference program's by a relative error of at most 0.0025.
The reference program's roundings to bfloat16 on the way count: a program that leaves them out, or rounds other values in their place, can miss the bound.
Values may be sent and summed in bfloat16 or wider, within the bound.
No kernel may reach another device: no remote copies, remote signals or barrier semaphores. Data moves between devices by JAX's collectives and lax.ppermute only.
A program may use at most 192 MiB of HBM per device.

```python
import math
import jax
import jax.numpy as jnp
from jax import lax

BANDS = 188
ATOMS = 2048
BLOCKS = 4
BLOCK_ROWS = 4
BLOCK_COLS = 32
MATCHES = 8
SLOTS = 2
ITERS = 2
HEIGHT = 128
WIDTH = 512
N_ROW = 8
N_COL = 16


def set_ends(array, rng, low, top_value):
    index_at = [jax.random.randint(jax.random.fold_in(rng, axis), (), 0, length) for axis, length in enumerate(array.shape)]
    main_axis = array.shape.index(max(array.shape))
    beside = index_at[:main_axis] + [(index_at[main_axis] + 1) % array.shape[main_axis]] + index_at[main_axis + 1:]
    return array.at[tuple(index_at)].set(low).at[tuple(beside)].set(top_value)


def level_of(key, shape, cuts, least, top_value):
    def one(position, shards_of):
        steps = jax.random.uniform(jax.random.fold_in(jax.random.fold_in(key, 6), position), (shards_of,), jnp.float32, least / len(cuts), top_value / len(cuts))
        return jnp.repeat(jnp.exp(steps), shape[position] // shards_of).reshape((-1,) + (1,) * (len(shape) - position - 1))

    loudness = one(*cuts[0])
    for cut in cuts[1:]:
        loudness = loudness * one(*cut)
    return loudness


def noise(key, dims, spread, limit, shards=(), kind=jnp.bfloat16):
    entries = spread * jax.random.normal(key, dims, jnp.float32)
    if shards:
        entries = entries * level_of(key, dims, shards, -0.22, 0.18)
    return jnp.clip(entries, -limit, limit).astype(kind)


def setup_inputs(seed: int = 0) -> dict:
    seeds = jax.random.split(jax.random.key(seed), 10)
    return {
        "observed": noise(seeds[0], (HEIGHT, WIDTH, BANDS), 1.0, 6.0, ((0, 8), (1, 16))),
        "library": noise(seeds[1], (BANDS, ATOMS), ATOMS ** -0.5, 0.125),
        "warm": jnp.clip(1.0 * jax.random.uniform(seeds[2], (HEIGHT, WIDTH, ATOMS), jnp.float32) ** level_of(seeds[2], (HEIGHT, WIDTH, ATOMS), ((0, 8), (1, 16)), -0.2, 0.2), 0.0, 1.0).astype(jnp.bfloat16),
        "match_peer": set_ends(jax.random.randint(seeds[3], (N_ROW * BLOCKS, N_COL, MATCHES), 0, N_COL), jax.random.fold_in(seeds[3], 1), 0, N_COL - 1).astype(jnp.int32),
        "match_slot": set_ends(jax.random.randint(seeds[4], (N_ROW * BLOCKS, N_COL, MATCHES), 0, SLOTS), jax.random.fold_in(seeds[4], 1), 0, SLOTS - 1).astype(jnp.int32),
        "match_count": set_ends(jax.random.randint(seeds[5], (N_ROW * BLOCKS, N_COL), 1, MATCHES + 1), jax.random.fold_in(seeds[5], 1), 1, MATCHES).astype(jnp.int32),
        "match_weight": jnp.clip(jnp.exp(math.log(10.0) - 4.6051702 * jax.random.uniform(seeds[6], (N_ROW * BLOCKS, N_COL, MATCHES), jnp.float32) ** level_of(seeds[6], (N_ROW * BLOCKS, N_COL, MATCHES), ((0, 8), (1, 16)), -0.2, 0.2)), 0.1, 10.0),
        "wanted": set_ends(jax.random.randint(seeds[7], (N_ROW, N_COL * N_COL, SLOTS), 0, BLOCKS), jax.random.fold_in(seeds[7], 1), 0, BLOCKS - 1).astype(jnp.int32),
        "threshold": jnp.clip(jnp.exp(jax.random.uniform(seeds[8], (ATOMS,), jnp.float32, math.log(0.02), math.log(0.2))), 0.02, 0.2),
    }


MU = 1.0
GAMMA = 0.6
ETA = 0.3

def coefficients(peer, slot, count, weight, group, slots):
    ranks = jnp.arange(weight.shape[1], dtype=jnp.int32)
    live = ranks[None, :] < count[:, None]
    masked = jnp.where(live, weight, 0.0)
    share = masked / jnp.sum(masked, axis=1, keepdims=True)
    column = peer * slots + slot
    targets = jnp.arange(group * slots, dtype=jnp.int32)
    onehot = column[:, :, None] == targets[None, None, :]
    return jnp.sum(jnp.where(onehot, share[:, :, None], 0.0), axis=1).astype(jnp.bfloat16)

def solve_step(base, tile, dual, library, chol):
    right = base + MU * (tile.astype(jnp.float32) + dual)
    small = jnp.dot(right.astype(jnp.bfloat16).astype(jnp.float32), library.T.astype(jnp.float32), preferred_element_type=jnp.float32)
    solved = jax.scipy.linalg.cho_solve((chol, True), small.T)
    back = jnp.dot(solved.T.astype(jnp.bfloat16).astype(jnp.float32), library.astype(jnp.float32), preferred_element_type=jnp.float32)
    return (right - back) / MU

def neighbours(beside_all):
    total = beside_all[:-2, 1:-1] + beside_all[2:, 1:-1] + beside_all[1:-1, :-2] + beside_all[1:-1, 2:]
    return 0.25 * total

def update(primal, dual, averaged, spatial, threshold):
    blend = (primal - dual + GAMMA * averaged + ETA * spatial) / (1.0 + GAMMA + ETA)
    fresh = jnp.maximum(blend - threshold[None, :], 0.0)
    return (fresh.astype(jnp.bfloat16), dual - primal + fresh)

def reference(observed, library, warm, match_peer, match_slot, match_count, match_weight, wanted, threshold):
    tile_rows = BLOCKS * BLOCK_ROWS
    pixels = tile_rows * BLOCK_COLS
    gram = jnp.dot(library.astype(jnp.float32), library.T.astype(jnp.float32), preferred_element_type=jnp.float32) + MU * jnp.eye(BANDS, dtype=jnp.float32)
    chol = jnp.linalg.cholesky(gram)
    dual = jnp.zeros((N_ROW * N_COL, pixels, ATOMS), jnp.float32)
    current = warm
    for step in range(ITERS):
        padded = jnp.pad(current, ((1, 1), (1, 1), (0, 0)))

        def device(packed):
            index, dual_here = packed
            row_pos = (index // N_COL).astype(jnp.int32)
            col_pos = (index % N_COL).astype(jnp.int32)
            top = row_pos * tile_rows
            left = col_pos * BLOCK_COLS
            anchor = jnp.zeros((), jnp.int32)
            seen = lax.dynamic_slice(observed, (top, left, anchor), (tile_rows, BLOCK_COLS, BANDS)).reshape(pixels, BANDS)
            tile = lax.dynamic_slice(current, (top, left, anchor), (tile_rows, BLOCK_COLS, ATOMS)).reshape(pixels, ATOMS)
            base = jnp.dot(seen.astype(jnp.float32), library.astype(jnp.float32), preferred_element_type=jnp.float32)
            primal = solve_step(base, tile, dual_here, library, chol)
            beside_all = lax.dynamic_slice(padded, (top, left, anchor), (tile_rows + 2, BLOCK_COLS + 2, ATOMS)).astype(jnp.float32)
            spatial = neighbours(beside_all).reshape(pixels, ATOMS)
            first = row_pos * BLOCKS
            peers = lax.dynamic_slice(match_peer, (first, col_pos, anchor), (BLOCKS, 1, MATCHES))[:, 0]
            places = lax.dynamic_slice(match_slot, (first, col_pos, anchor), (BLOCKS, 1, MATCHES))[:, 0]
            counts = lax.dynamic_slice(match_count, (first, col_pos), (BLOCKS, 1))[:, 0]
            weights = lax.dynamic_slice(match_weight, (first, col_pos, anchor), (BLOCKS, 1, MATCHES))[:, 0]
            coef = coefficients(peers, places, counts, weights, N_COL, SLOTS)
            asked = lax.dynamic_slice(wanted, (row_pos, col_pos * N_COL, anchor), (1, N_COL, SLOTS))[0]

            def fetch(peer_col, block):
                starts = (top + block * BLOCK_ROWS, (peer_col * BLOCK_COLS).astype(jnp.int32), anchor)
                return lax.dynamic_slice(current, starts, (BLOCK_ROWS, BLOCK_COLS, ATOMS))
            fetched = jax.vmap(jax.vmap(fetch, (None, 0)), (0, 0))(jnp.arange(N_COL, dtype=jnp.int32), asked)
            averaged = jnp.dot(coef.astype(jnp.float32), fetched.reshape(N_COL * SLOTS, -1).astype(jnp.float32), preferred_element_type=jnp.float32)
            return update(primal, dual_here, averaged.reshape(pixels, ATOMS), spatial, threshold)
        fresh, dual = lax.map(device, (jnp.arange(N_ROW * N_COL, dtype=jnp.int32), dual))
        fresh = fresh.reshape(N_ROW, N_COL, tile_rows, BLOCK_COLS, ATOMS)
        current = fresh.transpose(0, 2, 1, 3, 4).reshape(HEIGHT, WIDTH, ATOMS)
    rebuilt = jnp.dot(current.reshape(-1, ATOMS).astype(jnp.float32), library.T.astype(jnp.float32), preferred_element_type=jnp.float32)
    misfit = observed.astype(jnp.float32) - rebuilt.reshape(HEIGHT, WIDTH, BANDS)
    return (current, misfit)
```

```python
import functools

import jax
import jax.numpy as jnp
from jax import lax
from jax.experimental import pallas as pl
from jax.experimental.pallas import tpu as pltpu
from jax.sharding import PartitionSpec as P

BLOCK_ROWS = 4
MU = 1.0
GAMMA = 0.6
ETA = 0.3
TOTAL = 1.0 + GAMMA + ETA
LANES = 128
BANDS_PAD = 256
CODE_SCALE = 64000.0
CODE_SHIFT = 32768.0
MIB = 1024 * 1024

F32 = jnp.float32
BF16 = jnp.bfloat16


def params(limit_mib):
    return pltpu.CompilerParams(vmem_limit_bytes=limit_mib * MIB)


def cost(flops, moved):
    return pl.CostEstimate(flops=flops, bytes_accessed=moved, transcendentals=0)


def times_transposed(left, right):
    return lax.dot_general(
        left, right, (((1,), (1,)), ((), ())), preferred_element_type=F32
    )


def encode_fixed(value):
    return jnp.round(value * CODE_SCALE - CODE_SHIFT).astype(jnp.int32).astype(jnp.int16)


def decode_fixed(code):
    return (code.astype(jnp.int32).astype(F32) + CODE_SHIFT) * (1.0 / CODE_SCALE)


def encode_float(value):
    return value.astype(BF16)


def decode_float(code):
    return code.astype(F32)


def spread_kernel(tile_ref, out_ref):
    for p in range(out_ref.shape[0]):
        out_ref[p] = tile_ref[:, p * LANES : (p + 1) * LANES]


def spread(tile, peers):
    pixels, atoms = tile.shape
    step = pixels // 8
    return pl.pallas_call(
        spread_kernel,
        grid=(8,),
        in_specs=[pl.BlockSpec((step, atoms), lambda i: (i, 0))],
        out_specs=pl.BlockSpec((peers, step, LANES), lambda i: (0, i, 0)),
        out_shape=jax.ShapeDtypeStruct((peers, pixels, LANES), tile.dtype),
        compiler_params=params(16),
        cost_estimate=cost(pixels * atoms, 4 * pixels * atoms),
        name="spread",
    )(tile)


def inverse_kernel(lib_ref, inv_ref):
    size = lib_ref.shape[0]
    lib = lib_ref[...]
    rows = lax.broadcasted_iota(jnp.int32, (size, size), 0)
    cols = lax.broadcasted_iota(jnp.int32, (size, size), 1)
    eye = (rows == cols).astype(F32)
    gram = times_transposed(lib, lib) + MU * eye
    bound = jnp.max(jnp.sum(jnp.abs(gram), axis=1, keepdims=True))
    inv_ref[...] = eye * (2.0 / (1.0 + bound))

    def exact(a, b):
        return jnp.dot(a, b, precision=lax.Precision.HIGHEST, preferred_element_type=F32)

    def unfinished(state):
        count, worst = state
        return jnp.logical_and(count < 22, worst > 1e-4)

    def improve(state):
        count, _ = state
        x = inv_ref[...]
        rest = eye - exact(gram, x)
        inv_ref[...] = x + exact(x, rest)
        return count + 1, jnp.max(jnp.sum(jnp.abs(rest), axis=1, keepdims=True))

    lax.while_loop(unfinished, improve, (jnp.int32(0), jnp.float32(1.0)))


def gram_inverse(lib):
    size = lib.shape[0]
    return pl.pallas_call(
        inverse_kernel,
        out_shape=jax.ShapeDtypeStruct((size, size), F32),
        compiler_params=params(16),
        cost_estimate=cost(10 * 12 * size**3, 4 * size * size),
        name="inverse",
    )(lib)


def solve_kernel(first, *refs):
    if first:
        obs, lib, inv, thr, z, up, down, left, right, parts, primal = refs[:11]
        padded, base, low, back = refs[11:]
    else:
        obs, lib, inv, thr, z, up, down, left, right, old_parts, old_primal, mix, parts = refs[:13]
        padded, base, low, back = refs[13:]
    i = pl.program_id(0)
    peers, pixels, _ = z.shape
    row = up.shape[1]
    block = obs.shape[0]

    @pl.when(i == 0)
    def _():
        padded[:, :row] = up[...]
        padded[:, row : row + pixels] = z[...]
        padded[:, row + pixels :] = down[...]

    at = pl.multiple_of(i * block, block)
    base[...] = jnp.dot(obs[...], lib[...], preferred_element_type=F32)
    for p in range(peers):
        lanes = slice(p * LANES, (p + 1) * LANES)
        value = base[:, lanes] + MU * padded[p, pl.ds(at + row, block), :].astype(F32)
        if not first:
            mixed = decode_fixed(mix[p])
            fresh = jnp.maximum(old_parts[:, lanes] + (GAMMA / TOTAL) * mixed, 0.0)
            value = value + MU * (fresh - old_primal[:, lanes])
        low[:, lanes] = value.astype(BF16)
    small = times_transposed(low[...], lib[...])
    solved = jnp.dot(
        small, inv[...], precision=lax.Precision.HIGHEST, preferred_element_type=F32
    )
    back[...] = jnp.dot(solved.astype(BF16), lib[...], preferred_element_type=F32)
    place = lax.broadcasted_iota(jnp.int32, (block, LANES), 0) % row
    for p in range(peers):
        lanes = slice(p * LANES, (p + 1) * LANES)
        here = padded[p, pl.ds(at + row, block), :].astype(F32)
        above = padded[p, pl.ds(at, block), :].astype(F32)
        below = padded[p, pl.ds(at + 2 * row, block), :].astype(F32)

        def edge(halo):
            return jnp.concatenate(
                [
                    jnp.broadcast_to(halo[0, k : k + 1, lanes], (row, LANES))
                    for k in range(block // row)
                ],
                axis=0,
            )

        before = jnp.where(place == 0, edge(left), pltpu.roll(here, 1, 0))
        after = jnp.where(place == row - 1, edge(right), pltpu.roll(here, block - 1, 0))
        spatial = 0.25 * (above + below + before + after)
        unmixed = (base[:, lanes] + MU * here - back[:, lanes]) / MU
        if first:
            primal[:, lanes] = unmixed
        parts[:, lanes] = (unmixed + ETA * spatial) * (1.0 / TOTAL) - thr[:, lanes]


def solve(first, obs, lib, inv, thr, z, halos, carried=()):
    peers, pixels, _ = z.shape
    atoms = lib.shape[1]
    up, down, left, right = halos
    row = up.shape[1]
    block = BLOCK_ROWS * row
    steps = pixels // block
    whole = lambda a: pl.BlockSpec(a.shape, lambda i, n=a.ndim: (0,) * n)
    tile = pl.BlockSpec((block, atoms), lambda i: (i, 0))
    piece = pl.BlockSpec((peers, block, LANES), lambda i: (0, i, 0))
    side = pl.BlockSpec((1, BLOCK_ROWS, atoms), lambda i: (i, 0, 0))
    full = jax.ShapeDtypeStruct((pixels, atoms), F32)
    return pl.pallas_call(
        functools.partial(solve_kernel, first),
        grid=(steps,),
        in_specs=[
            pl.BlockSpec((block, obs.shape[1]), lambda i: (i, 0)),
            whole(lib), whole(inv), whole(thr), whole(z), whole(up), whole(down), side, side,
        ]
        + ([] if first else [tile, tile, piece]),
        out_specs=[tile, tile] if first else tile,
        out_shape=[full, full] if first else full,
        scratch_shapes=[
            pltpu.VMEM((peers, pixels + 2 * row, LANES), BF16),
            pltpu.VMEM((block, atoms), F32),
            pltpu.VMEM((block, atoms), BF16),
            pltpu.VMEM((block, atoms), F32),
        ],
        compiler_params=params(34),
        cost_estimate=cost(6 * pixels * atoms * BANDS_PAD, 16 * pixels * atoms),
        name="solve_first" if first else "solve_second",
    )(obs, lib, inv, thr, z, up, down, left, right, *carried)


def mix_kernel(encode, matches, place_ref, weight_ref, z_ref, out_ref):
    def one(t, carry):
        total = None
        for k in range(matches):
            term = z_ref[place_ref[t * matches + k]].astype(F32) * weight_ref[t * matches + k]
            total = term if total is None else total + term
        out_ref[t] = encode(total)
        return carry

    lax.fori_loop(0, out_ref.shape[0], one, 0)


def mix(encode, dtype, place, weight, z, matches, block):
    peers, pixels, _ = z.shape
    blocks = peers * pixels // block
    out = pl.pallas_call(
        functools.partial(mix_kernel, encode, matches),
        in_specs=[
            pl.BlockSpec(memory_space=pltpu.SMEM),
            pl.BlockSpec(memory_space=pltpu.SMEM),
            pl.BlockSpec(memory_space=pltpu.VMEM),
        ],
        out_specs=pl.BlockSpec(memory_space=pltpu.VMEM),
        out_shape=jax.ShapeDtypeStruct((blocks, block, LANES), dtype),
        compiler_params=params(16),
        cost_estimate=cost(2 * matches * blocks * block * LANES, 4 * blocks * block * LANES),
        name="mix",
    )(place, weight, z.reshape(blocks, block, LANES))
    return out.reshape(peers, pixels, LANES)


def fresh_kernel(parts, mix_ref, out_ref):
    for p in range(out_ref.shape[0]):
        lanes = slice(p * LANES, (p + 1) * LANES)
        mixed = decode_fixed(mix_ref[p])
        out_ref[p] = jnp.maximum(parts[:, lanes] + (GAMMA / TOTAL) * mixed, 0.0).astype(BF16)


def fresh_pieces(parts, mixed):
    peers, pixels, _ = mixed.shape
    atoms = parts.shape[1]
    step = pixels // 8
    piece = pl.BlockSpec((peers, step, LANES), lambda i: (0, i, 0))
    return pl.pallas_call(
        fresh_kernel,
        grid=(8,),
        in_specs=[pl.BlockSpec((step, atoms), lambda i: (i, 0)), piece],
        out_specs=piece,
        out_shape=jax.ShapeDtypeStruct((peers, pixels, LANES), BF16),
        compiler_params=params(16),
        cost_estimate=cost(4 * pixels * atoms, 8 * pixels * atoms),
        name="fresh",
    )(parts, mixed)


def final_kernel(parts, mix_ref, obs, lib, out_ref, misfit_ref):
    for p in range(mix_ref.shape[0]):
        lanes = slice(p * LANES, (p + 1) * LANES)
        mixed = decode_float(mix_ref[p])
        out_ref[:, lanes] = jnp.maximum(
            parts[:, lanes] + (GAMMA / TOTAL) * mixed, 0.0
        ).astype(BF16)
    rebuilt = times_transposed(out_ref[...], lib[...])
    misfit_ref[...] = (obs[...].astype(F32) - rebuilt)[:, : misfit_ref.shape[1]]


def final(parts, mixed, obs, lib, bands):
    peers, pixels, _ = mixed.shape
    atoms = parts.shape[1]
    step = pixels // 4
    tile = lambda n: pl.BlockSpec((step, n), lambda i: (i, 0))
    return pl.pallas_call(
        final_kernel,
        grid=(4,),
        in_specs=[
            tile(atoms),
            pl.BlockSpec((peers, step, LANES), lambda i: (0, i, 0)),
            tile(obs.shape[1]),
            pl.BlockSpec(lib.shape, lambda i: (0, 0)),
        ],
        out_specs=[tile(atoms), tile(bands)],
        out_shape=[
            jax.ShapeDtypeStruct((pixels, atoms), BF16),
            jax.ShapeDtypeStruct((pixels, bands), F32),
        ],
        compiler_params=params(16),
        cost_estimate=cost(2 * pixels * atoms * BANDS_PAD, 8 * pixels * atoms),
        name="final",
    )(parts, mixed, obs, lib)


def match_table(peer, slot, count, weight, wanted, blocks):
    matches = weight.shape[1]
    slots = wanted.shape[1]
    ranks = jnp.arange(matches, dtype=jnp.int32)
    masked = jnp.where(ranks[None, :] < count[:, None], weight, 0.0)
    share = masked / jnp.sum(masked, axis=1, keepdims=True)
    column = peer * slots + slot
    same = column[:, :, None] == column[:, None, :]
    merged = jnp.sum(jnp.where(same, share[:, None, :], 0.0), axis=2).astype(BF16).astype(F32)
    again = jnp.any(same & (ranks[None, None, :] < ranks[None, :, None]), axis=2)
    coef = jnp.where(again, 0.0, merged)
    asked = wanted.reshape(-1)
    targets = jnp.arange(asked.shape[0], dtype=jnp.int32)
    chosen = jnp.sum(
        jnp.where(column[:, :, None] == targets[None, None, :], asked[None, None, :], 0), axis=2
    )
    place = peer * blocks + chosen
    return jnp.concatenate([coef.reshape(-1), place.astype(F32).reshape(-1)])


def shifted(array, axis, up):
    peers = lax.axis_size(axis)
    pairs = [(k, k + 1) for k in range(peers - 1)]
    return lax.ppermute(array, axis, pairs if up else [(b, a) for a, b in pairs])


def exchanged(pieces):
    return lax.all_to_all(pieces, "col", 0, 0, tiled=True)


def side_rows(column, blocks):
    atoms = column.shape[-1]
    return column.astype(F32).reshape(blocks, -1, atoms)


def local(
    observed, library, warm, match_peer, match_slot, match_count, match_weight, wanted, threshold
):
    tile_rows, tile_cols, atoms = warm.shape
    bands = library.shape[0]
    pixels = tile_rows * tile_cols
    blocks = tile_rows // BLOCK_ROWS
    block = BLOCK_ROWS * tile_cols
    peers = lax.axis_size("col")
    matches = match_weight.shape[2]

    pieces = spread(warm.reshape(pixels, atoms), peers)
    strip = exchanged(pieces)

    table = match_table(
        match_peer[:, 0], match_slot[:, 0], match_count[:, 0], match_weight[:, 0], wanted[0], blocks
    )
    tables = lax.all_gather(table, "col")
    half = table.shape[0] // 2
    weight = tables[:, :half].reshape(-1)
    place = tables[:, half:].astype(jnp.int32).reshape(-1)

    halos = (
        shifted(pieces[:, pixels - tile_cols :], "row", True),
        shifted(pieces[:, :tile_cols], "row", False),
        side_rows(shifted(warm[:, -1], "col", True), blocks),
        side_rows(shifted(warm[:, 0], "col", False), blocks),
    )
    lib = jnp.pad(library, ((0, BANDS_PAD - bands), (0, 0)))
    obs = jnp.pad(observed.reshape(pixels, bands), ((0, 0), (0, BANDS_PAD - bands)))
    inv = gram_inverse(lib)
    thr = threshold[None, :]
    parts, primal = solve(True, obs, lib, inv, thr, pieces, halos)

    mixed = exchanged(mix(encode_fixed, jnp.int16, place, weight, strip, matches, block))
    pieces = fresh_pieces(parts, mixed)
    strip = exchanged(pieces)

    sides = pieces.reshape(peers, tile_rows, tile_cols, LANES)
    by_row = lambda a: jnp.moveaxis(a, 0, 1).reshape(tile_rows, atoms)
    halos = (
        shifted(pieces[:, pixels - tile_cols :], "row", True),
        shifted(pieces[:, :tile_cols], "row", False),
        side_rows(by_row(shifted(sides[:, :, -1], "col", True)), blocks),
        side_rows(by_row(shifted(sides[:, :, 0], "col", False)), blocks),
    )
    parts = solve(False, obs, lib, inv, thr, pieces, halos, (parts, primal, mixed))

    mixed = exchanged(mix(encode_float, BF16, place, weight, strip, matches, block))
    abundance, misfit = final(parts, mixed, obs, lib, bands)
    return (
        abundance.reshape(tile_rows, tile_cols, atoms),
        misfit.reshape(tile_rows, tile_cols, bands),
    )


def solution(mesh):
    return jax.shard_map(
        local,
        mesh=mesh,
        in_specs=(
            P("row", "col", None),
            P(),
            P("row", "col", None),
            P("row", "col", None),
            P("row", "col", None),
            P("row", "col"),
            P("row", "col", None),
            P("row", "col", None),
            P(),
        ),
        out_specs=(P("row", "col", None), P("row", "col", None)),
        check_vma=False,
    )
```

```python
import functools

import jax
import jax.numpy as jnp
from jax import lax
from jax.experimental import pallas as pl
from jax.experimental.pallas import tpu as pltpu
from jax.sharding import PartitionSpec as P


BLOCK_ROWS = 4
MU = 1.0
GAMMA = 0.6
ETA = 0.3
TOTAL = 1.0 + GAMMA + ETA
LANES = 128
BANDS_PAD = 256
CODE_SCALE = 64000.0
CODE_SHIFT = 32768.0
GROUP = 8
STEPS = 8
WIDE = 2
TABLE_ROWS = 16
MIB = 1024 * 1024

F32 = jnp.float32
BF16 = jnp.bfloat16


def cost(flops, moved):
    return pl.CostEstimate(flops=flops, bytes_accessed=moved, transcendentals=0)


def times_transposed(left, right):
    return lax.dot_general(
        left, right, (((1,), (1,)), ((), ())), preferred_element_type=F32
    )


def encode_fixed(value):
    return jnp.round(value * CODE_SCALE - CODE_SHIFT).astype(jnp.int32).astype(jnp.int16)


def decode_fixed(code):
    return (code.astype(jnp.int32).astype(F32) + CODE_SHIFT) * (1.0 / CODE_SCALE)


def encode_float(value):
    return value.astype(BF16)


def decode_float(code):
    return code.astype(F32)


def spread_kernel(
    blocks, asked_at, peer_at, slot_at, count_at, weight_at, tile, out,
    held, asked, peer, slot, count, weight, rows, table, small, come, go, extra,
):
    peers, pixels, _ = held.shape
    tables = (
        (asked_at, asked), (peer_at, peer), (slot_at, slot), (count_at, count), (weight_at, weight),
    )
    for k, (source, target) in enumerate(tables):
        pltpu.make_async_copy(source, target, small.at[k]).start()
    for p in range(peers):
        lanes = pl.ds(p * LANES, LANES)
        pltpu.make_async_copy(tile.at[:, lanes], held.at[p], come.at[p]).start()
    for k, (source, target) in enumerate(tables):
        pltpu.make_async_copy(source, target, small.at[k]).wait()
    slots = asked.shape[1]
    matches = weight.shape[2]
    ranks = lax.broadcasted_iota(jnp.int32, (1, matches), 1)
    rows[...] = jnp.zeros_like(rows)
    for j in range(weight.shape[0]):
        masked = jnp.where(ranks < count[:, j : j + 1], weight[j], 0.0)
        share = masked / jnp.sum(masked, axis=1, keepdims=True)
        column = peer[j] * slots + slot[j]
        total = jnp.zeros_like(share)
        again = jnp.zeros_like(share)
        for k in range(matches):
            same = column == column[:, k : k + 1]
            total = total + jnp.where(same, share[:, k : k + 1], 0.0)
            again = again + jnp.where(jnp.logical_and(same, ranks > k), 1.0, 0.0)
        chosen = jnp.zeros_like(column)
        for q in range(peers):
            for k in range(slots):
                named = asked[0, k : k + 1, q : q + 1]
                chosen = chosen + jnp.where(column == q * slots + k, named, 0)
        place = peer[j] * blocks + chosen
        rows[j : j + 1, :matches] = jnp.where(again > 0.0, 0.0, total)
        at = j + weight.shape[0]
        rows[at : at + 1, :matches] = place.astype(F32)
    table[...] = rows[...].astype(BF16)
    for p in range(peers):
        pltpu.make_async_copy(table, out.at[p, pl.ds(pixels, TABLE_ROWS), :], extra.at[p]).start()
    for p in range(peers):
        lanes = pl.ds(p * LANES, LANES)
        pltpu.make_async_copy(tile.at[:, lanes], held.at[p], come.at[p]).wait()
        pltpu.make_async_copy(held.at[p], out.at[p, pl.ds(0, pixels), :], go.at[p]).start()
    for p in range(peers):
        pltpu.make_async_copy(table, out.at[p, pl.ds(pixels, TABLE_ROWS), :], extra.at[p]).wait()
        pltpu.make_async_copy(held.at[p], out.at[p, pl.ds(0, pixels), :], go.at[p]).wait()


def spread(tile, peers, peer, slot, count, weight, wanted):
    pixels, atoms = tile.shape
    inputs = (wanted.transpose(0, 2, 1), peer, slot, count.T, weight, tile)
    inputs = tuple(pltpu.with_memory_space_constraint(a, pltpu.HBM) for a in inputs)
    return pl.pallas_call(
        functools.partial(spread_kernel, weight.shape[0]),
        in_specs=[pl.BlockSpec(memory_space=pltpu.HBM)] * len(inputs),
        out_specs=pl.BlockSpec(memory_space=pltpu.HBM),
        out_shape=pltpu.HBM((peers, pixels + TABLE_ROWS, LANES), tile.dtype),
        scratch_shapes=[
            pltpu.VMEM((peers, pixels, LANES), tile.dtype),
            *(pltpu.VMEM(a.shape, a.dtype) for a in inputs[:-1]),
            pltpu.VMEM((TABLE_ROWS, LANES), F32),
            pltpu.VMEM((TABLE_ROWS, LANES), BF16),
            pltpu.SemaphoreType.DMA((len(inputs) - 1,)),
            pltpu.SemaphoreType.DMA((peers,)),
            pltpu.SemaphoreType.DMA((peers,)),
            pltpu.SemaphoreType.DMA((peers,)),
        ],
        compiler_params=pltpu.CompilerParams(vmem_limit_bytes=16 * MIB),
        cost_estimate=cost(pixels * atoms, 4 * pixels * atoms),
        name="spread",
    )(*inputs)


def inverse_kernel(lib_ref, inv_ref):
    size = lib_ref.shape[0]
    lib = lib_ref[...]
    rows = lax.broadcasted_iota(jnp.int32, (size, size), 0)
    cols = lax.broadcasted_iota(jnp.int32, (size, size), 1)
    eye = (rows == cols).astype(F32)
    gram = times_transposed(lib, lib) + MU * eye
    bound = jnp.max(jnp.sum(jnp.abs(gram), axis=1, keepdims=True))
    inv_ref[...] = eye * (2.0 / (1.0 + bound))

    def exact(a, b):
        return jnp.dot(a, b, precision=lax.Precision.HIGHEST, preferred_element_type=F32)

    def unfinished(state):
        count, worst = state
        return jnp.logical_and(count < 22, worst > 1e-4)

    def improve(state):
        count, _ = state
        x = inv_ref[...]
        rest = eye - exact(gram, x)
        inv_ref[...] = x + exact(x, rest)
        return count + 1, jnp.max(jnp.sum(jnp.abs(rest), axis=1, keepdims=True))

    lax.while_loop(unfinished, improve, (jnp.int32(0), jnp.float32(1.0)))


def gram_inverse(lib):
    size = lib.shape[0]
    return pl.pallas_call(
        inverse_kernel,
        out_shape=jax.ShapeDtypeStruct((size, size), F32),
        cost_estimate=cost(10 * 12 * size**3, 4 * size * size),
        compiler_params=pltpu.CompilerParams(vmem_limit_bytes=63 * MIB),
        name="inverse",
    )(lib)


def solve_kernel(first, *refs):
    if first:
        obs, lib, inv, thr, z, up, down, left, right, parts, primal = refs[:11]
        padded, base, low, back = refs[11:]
    else:
        obs, lib, inv, thr, z, up, down, left, right, old_parts, old_primal, mix, parts = refs[:13]
        padded, base, low, back = refs[13:]
    i = pl.program_id(0)
    peers, pixels, _ = z.shape
    row = up.shape[1]
    block = obs.shape[0]
    pixels = padded.shape[1] - 2 * row

    @pl.when(i == 0)
    def _():
        padded[:, :row] = up[...]
        padded[:, row : row + pixels] = z[:, :pixels]
        padded[:, row + pixels :] = down[...]

    at = pl.multiple_of(i * block, block)
    base[...] = jnp.dot(obs[...], lib[...], preferred_element_type=F32)
    for p in range(peers):
        lanes = slice(p * LANES, (p + 1) * LANES)
        value = base[:, lanes] + MU * padded[p, pl.ds(at + row, block), :].astype(F32)
        if not first:
            mixed = decode_fixed(mix[p])
            fresh = jnp.maximum(old_parts[:, lanes] + (GAMMA / TOTAL) * mixed, 0.0)
            value = value + MU * (fresh - old_primal[:, lanes])
        low[:, lanes] = value.astype(BF16)
    small = times_transposed(low[...], lib[...])
    solved = jnp.dot(
        small, inv[...], precision=lax.Precision.HIGHEST, preferred_element_type=F32
    )
    back[...] = jnp.dot(solved.astype(BF16), lib[...], preferred_element_type=F32)
    place = lax.broadcasted_iota(jnp.int32, (block, LANES), 0) % row
    for p in range(peers):
        lanes = slice(p * LANES, (p + 1) * LANES)
        here = padded[p, pl.ds(at + row, block), :].astype(F32)
        above = padded[p, pl.ds(at, block), :].astype(F32)
        below = padded[p, pl.ds(at + 2 * row, block), :].astype(F32)

        def edge(halo):
            return jnp.concatenate(
                [
                    jnp.broadcast_to(halo[0, k : k + 1, lanes], (row, LANES))
                    for k in range(block // row)
                ],
                axis=0,
            )

        before = jnp.where(place == 0, edge(left), pltpu.roll(here, 1, 0))
        after = jnp.where(place == row - 1, edge(right), pltpu.roll(here, block - 1, 0))
        spatial = 0.25 * (above + below + before + after)
        unmixed = (base[:, lanes] + MU * here - back[:, lanes]) / MU
        if first:
            primal[:, lanes] = unmixed
        parts[:, lanes] = (unmixed + ETA * spatial) * (1.0 / TOTAL) - thr[:, lanes]


def solve(first, obs, lib, inv, thr, z, halos, carried=()):
    peers = z.shape[0]
    pixels = obs.shape[0]
    atoms = lib.shape[1]
    up, down, left, right = halos
    row = up.shape[1]
    block = BLOCK_ROWS * row
    steps = pixels // block
    whole = lambda a: pl.BlockSpec(a.shape, lambda i, n=a.ndim: (0,) * n)
    tile = pl.BlockSpec((block, atoms), lambda i: (i, 0))
    piece = pl.BlockSpec((peers, block, LANES), lambda i: (0, i, 0))
    side = pl.BlockSpec((1, BLOCK_ROWS, atoms), lambda i: (i, 0, 0))
    full = jax.ShapeDtypeStruct((pixels, atoms), F32)
    return pl.pallas_call(
        functools.partial(solve_kernel, first),
        grid=(steps,),
        in_specs=[
            pl.BlockSpec((block, obs.shape[1]), lambda i: (i, 0)),
            whole(lib), whole(inv), whole(thr), whole(z), whole(up), whole(down), side, side,
        ]
        + ([] if first else [tile, tile, piece]),
        out_specs=[tile, tile] if first else tile,
        out_shape=[full, full] if first else full,
        scratch_shapes=[
            pltpu.VMEM((peers, pixels + 2 * row, LANES), BF16),
            pltpu.VMEM((block, atoms), F32),
            pltpu.VMEM((block, atoms), BF16),
            pltpu.VMEM((block, atoms), F32),
        ],
        cost_estimate=cost(6 * pixels * atoms * BANDS_PAD, 16 * pixels * atoms),
        compiler_params=pltpu.CompilerParams(vmem_limit_bytes=63 * MIB),
        name="solve_first" if first else "solve_second",
    )(obs, lib, inv, thr, z, up, down, left, right, *carried)


def mix_kernel(encode, matches, place_ref, weight_ref, z_ref, out_ref):
    first = pl.program_id(0) * out_ref.shape[0]
    block = out_ref.shape[1]
    per = z_ref.shape[1] // block

    def one(t, carry):
        total = None
        for k in range(matches):
            at = (first + t) * matches + k
            place = place_ref[at]
            rows = pl.ds(pl.multiple_of((place % per) * block, block), block)
            term = z_ref[place // per, rows, :].astype(F32) * weight_ref[at]
            total = term if total is None else total + term
        out_ref[t] = encode(total)
        return carry

    lax.fori_loop(0, out_ref.shape[0], one, 0)


def mix(encode, dtype, place, weight, z, matches, block):
    peers = z.shape[0]
    pixels = z.shape[1] // block * block
    blocks = peers * pixels // block
    out = pl.pallas_call(
        functools.partial(mix_kernel, encode, matches),
        grid=(blocks // GROUP,),
        in_specs=[
            pl.BlockSpec(memory_space=pltpu.SMEM),
            pl.BlockSpec(memory_space=pltpu.SMEM),
            pl.BlockSpec(memory_space=pltpu.VMEM),
        ],
        out_specs=pl.BlockSpec((GROUP, block, LANES), lambda i: (i, 0, 0)),
        out_shape=pltpu.HBM((blocks, block, LANES), dtype),
        cost_estimate=cost(2 * matches * blocks * block * LANES, 4 * blocks * block * LANES),
        compiler_params=pltpu.CompilerParams(vmem_limit_bytes=48 * MIB),
        name="mix",
    )(place, weight, z)
    return out.reshape(peers, pixels, LANES)


def fresh_kernel(parts, mixed, out, held, code, made, come, came, go):
    step = parts.shape[0] // STEPS
    reads, writes = [], []
    for i in range(STEPS):
        at = pl.ds(i * step, step)
        reads.append(
            (
                pltpu.make_async_copy(parts.at[at, :], held.at[at, :], come.at[i]),
                pltpu.make_async_copy(mixed.at[:, at, :], code.at[:, at, :], came.at[i]),
            )
        )
        writes.append(pltpu.make_async_copy(made.at[:, at, :], out.at[:, at, :], go.at[i]))
    for pair in reads:
        for copy in pair:
            copy.start()
    for i in range(STEPS):
        for copy in reads[i]:
            copy.wait()
        at = pl.ds(i * step, step)
        for p in range(out.shape[0]):
            lanes = slice(p * LANES, (p + 1) * LANES)
            value = held[at, lanes] + (GAMMA / TOTAL) * decode_fixed(code[p, at, :])
            made[p, at, :] = jnp.maximum(value, 0.0).astype(BF16)
        writes[i].start()
    for copy in writes:
        copy.wait()


def fresh_pieces(parts, mixed):
    peers, pixels, _ = mixed.shape
    atoms = parts.shape[1]
    hbm = pl.BlockSpec(memory_space=pltpu.HBM)
    return pl.pallas_call(
        fresh_kernel,
        in_specs=[hbm, hbm],
        out_specs=hbm,
        out_shape=pltpu.HBM((peers, pixels, LANES), BF16),
        scratch_shapes=[
            pltpu.VMEM((pixels, atoms), F32),
            pltpu.VMEM((peers, pixels, LANES), mixed.dtype),
            pltpu.VMEM((peers, pixels, LANES), BF16),
            pltpu.SemaphoreType.DMA((STEPS,)),
            pltpu.SemaphoreType.DMA((STEPS,)),
            pltpu.SemaphoreType.DMA((STEPS,)),
        ],
        compiler_params=pltpu.CompilerParams(vmem_limit_bytes=63 * MIB),
        cost_estimate=cost(4 * pixels * atoms, 8 * pixels * atoms),
        name="fresh",
    )(parts, mixed)


def final_kernel(
    parts, mixed, obs, turned, out, misfit,
    held, code, made, rest, seen, spectra, come, came, go, went, side,
):
    step = parts.shape[0] // STEPS
    wide = WIDE * step
    reads, writes = [], []
    for i in range(STEPS):
        at = pl.ds(i * step, step)
        reads.append(
            (
                pltpu.make_async_copy(parts.at[at, :], held.at[at, :], come.at[i]),
                pltpu.make_async_copy(mixed.at[:, at, :], code.at[:, at, :], came.at[i]),
            )
        )
        writes.append(pltpu.make_async_copy(made.at[at, :], out.at[at, :], go.at[i]))
    others = (
        pltpu.make_async_copy(turned, spectra, side.at[0]),
        pltpu.make_async_copy(obs, seen, side.at[1]),
    )
    for i, pair in enumerate(reads):
        for copy in pair:
            copy.start()
        if i == 0:
            for copy in others:
                copy.start()
    for i in range(STEPS):
        for copy in reads[i]:
            copy.wait()
        at = pl.ds(i * step, step)
        for p in range(mixed.shape[0]):
            lanes = slice(p * LANES, (p + 1) * LANES)
            value = held[at, lanes] + (GAMMA / TOTAL) * decode_float(code[p, at, :])
            made[at, lanes] = jnp.maximum(value, 0.0).astype(BF16)
        writes[i].start()
        if i == 0:
            for copy in others:
                copy.wait()
        if (i + 1) % WIDE == 0:
            k = i // WIDE
            rows = pl.ds(k * wide, wide)
            rebuilt = jnp.dot(made[rows, :], spectra[...], preferred_element_type=F32)
            rest[rows, :] = (seen[rows, :].astype(F32) - rebuilt)[:, : rest.shape[1]]
            writes.append(
                pltpu.make_async_copy(rest.at[rows, :], misfit.at[rows, :], went.at[k])
            )
            writes[-1].start()
    for copy in writes:
        copy.wait()


def final(parts, mixed, obs, turned, bands):
    peers, pixels, _ = mixed.shape
    atoms = parts.shape[1]
    hbm = pl.BlockSpec(memory_space=pltpu.HBM)
    return pl.pallas_call(
        final_kernel,
        in_specs=[hbm, hbm, hbm, hbm],
        out_specs=[hbm, hbm],
        out_shape=[pltpu.HBM((pixels, atoms), BF16), pltpu.HBM((pixels, bands), F32)],
        scratch_shapes=[
            pltpu.VMEM((pixels, atoms), F32),
            pltpu.VMEM((peers, pixels, LANES), mixed.dtype),
            pltpu.VMEM((pixels, atoms), BF16),
            pltpu.VMEM((pixels, bands), F32),
            pltpu.VMEM(obs.shape, obs.dtype),
            pltpu.VMEM(turned.shape, turned.dtype),
            pltpu.SemaphoreType.DMA((STEPS,)),
            pltpu.SemaphoreType.DMA((STEPS,)),
            pltpu.SemaphoreType.DMA((STEPS,)),
            pltpu.SemaphoreType.DMA((STEPS // WIDE,)),
            pltpu.SemaphoreType.DMA((2,)),
        ],
        compiler_params=pltpu.CompilerParams(vmem_limit_bytes=63 * MIB),
        cost_estimate=cost(2 * pixels * atoms * BANDS_PAD, 8 * pixels * atoms),
        name="final",
    )(parts, mixed, obs, turned)


def shifted(array, axis, up):
    peers = lax.axis_size(axis)
    pairs = [(k, k + 1) for k in range(peers - 1)]
    return lax.ppermute(array, axis, pairs if up else [(b, a) for a, b in pairs])


def exchanged(pieces):
    return lax.all_to_all(pieces, "col", 0, 0, tiled=True)


def shifted_edges(pieces, tile_rows, tile_cols):
    peers = pieces.shape[0]
    pixels = tile_rows * tile_cols
    sides = pieces[:, :pixels].reshape(peers, tile_rows, tile_cols, LANES)
    up = shifted(pieces[:, pixels - tile_cols : pixels], "row", True)
    down = shifted(pieces[:, :tile_cols], "row", False)
    left = shifted(sides[:, :, -1], "col", True)
    right = shifted(sides[:, :, 0], "col", False)

    def side_rows(column):
        rows = jnp.moveaxis(column.astype(F32), 0, 1)
        return rows.reshape(tile_rows // BLOCK_ROWS, BLOCK_ROWS, -1)

    return up, down, side_rows(left), side_rows(right)


def local(
    observed, library, warm, match_peer, match_slot, match_count, match_weight, wanted, threshold
):
    tile_rows, tile_cols, atoms = warm.shape
    bands = library.shape[0]
    pixels = tile_rows * tile_cols
    blocks = tile_rows // BLOCK_ROWS
    block = BLOCK_ROWS * tile_cols
    peers = lax.axis_size("col")
    matches = match_weight.shape[2]

    pieces = spread(
        warm.reshape(pixels, atoms), peers,
        match_peer, match_slot, match_count, match_weight, wanted,
    )
    strip = exchanged(pieces)
    halos = shifted_edges(pieces, tile_rows, tile_cols)
    lib = jnp.pad(library, ((0, BANDS_PAD - bands), (0, 0)))
    obs = jnp.pad(observed.reshape(pixels, bands), ((0, 0), (0, BANDS_PAD - bands)))
    inv = gram_inverse(lib)
    thr = threshold[None, :]

    tables = strip[:, pixels : pixels + 2 * blocks, :matches].astype(F32)
    weight = tables[:, :blocks].reshape(-1)
    place = tables[:, blocks:].astype(jnp.int32).reshape(-1)
    sums = mix(encode_fixed, jnp.int16, place, weight, strip, matches, block)
    mixed = exchanged(sums)
    parts, primal = solve(True, obs, lib, inv, thr, pieces, halos)
    pieces = fresh_pieces(parts, mixed)
    strip = exchanged(pieces)
    halos = shifted_edges(pieces, tile_rows, tile_cols)
    sums = mix(encode_float, BF16, place, weight, strip, matches, block)
    mixed_again = exchanged(sums)
    parts = solve(False, obs, lib, inv, thr, pieces, halos, (parts, primal, mixed))
    abundance, misfit = final(parts, mixed_again, obs, lib.T, bands)
    return (
        abundance.reshape(tile_rows, tile_cols, atoms),
        misfit.reshape(tile_rows, tile_cols, bands),
    )


def solution(mesh):
    return jax.shard_map(
        local,
        mesh=mesh,
        in_specs=(
            P("row", "col", None),
            P(),
            P("row", "col", None),
            P("row", "col", None),
            P("row", "col", None),
            P("row", "col"),
            P("row", "col", None),
            P("row", "col", None),
            P(),
        ),
        out_specs=(P("row", "col", None), P("row", "col", None)),
        check_vma=False,
    )
```

```python
import functools

import jax
import jax.numpy as jnp
from jax import lax
from jax.experimental import pallas as pl
from jax.experimental.pallas import tpu as pltpu
from jax.sharding import PartitionSpec as P


BLOCK_ROWS = 4
BLOCKS = 4
MU = 1.0
GAMMA = 0.6
ETA = 0.3
TOTAL = 1.0 + GAMMA + ETA
LANES = 128
BANDS_PAD = 192
CODE_SCALE = 64000.0
CODE_SHIFT = 32768.0
STEPS = 8
AHEAD = 5
WIDE = 2
TABLE_ROWS = 16
MIB = 1024 * 1024

F32 = jnp.float32
BF16 = jnp.bfloat16


def cost(flops, moved):
    return pl.CostEstimate(flops=flops, bytes_accessed=moved, transcendentals=0)


def times_transposed(left, right):
    return lax.dot_general(
        left, right, (((1,), (1,)), ((), ())), preferred_element_type=F32
    )


def encode_fixed(value):
    return jnp.round(value * CODE_SCALE - CODE_SHIFT).astype(jnp.int32).astype(jnp.int16)


def decode_fixed(code):
    return (code.astype(jnp.int32).astype(F32) + CODE_SHIFT) * (1.0 / CODE_SCALE)


def encode_float(value):
    return value.astype(BF16)


def decode_float(code):
    return code.astype(F32)


def swapped(a, b):
    low = lax.broadcasted_iota(jnp.int32, a.shape, 1) < 4
    first = jnp.where(low, a, pltpu.roll(b, 4, 1))
    second = jnp.where(low, pltpu.roll(a, 4, 1), b)
    return first, second


def weave(parts):
    f0, s0 = swapped(parts[0], parts[1])
    f1, s1 = swapped(parts[2], parts[3])
    tiles = [t[v] for v in range(f0.shape[0]) for t in (f0, f1, s0, s1)]
    return jnp.concatenate(tiles, axis=0)


def unweave(rows):
    tiles = rows.reshape(-1, 4, 8, LANES)
    b0, b1 = swapped(tiles[:, 0], tiles[:, 2])
    b2, b3 = swapped(tiles[:, 1], tiles[:, 3])
    return b0, b1, b2, b3


def halves(rows):
    return rows.reshape(-1, 8, LANES)


def spread_kernel(
    asked_at, peer_at, slot_at, count_at, weight_at, tile, out,
    held, made, asked, peer, slot, count, weight, rows, table, small, come, go, extra,
):
    blocks, block, _ = held.shape
    peers = made.shape[0]
    pixels = blocks * block
    step = block // STEPS
    for i in range(STEPS):
        at = pl.ds(i * step, step)
        pltpu.make_async_copy(tile.at[:, at, :], held.at[:, at, :], come.at[i]).start()
    tables = (
        (asked_at, asked), (peer_at, peer), (slot_at, slot), (count_at, count), (weight_at, weight),
    )
    for k, (source, target) in enumerate(tables):
        pltpu.make_async_copy(source, target, small.at[k]).start()
    for k, (source, target) in enumerate(tables):
        pltpu.make_async_copy(source, target, small.at[k]).wait()
    slots = asked.shape[1]
    matches = weight.shape[2]
    stacked = lambda ref: jnp.concatenate([ref[j] for j in range(blocks)], axis=0)
    peer, slot, weight = stacked(peer), stacked(slot), stacked(weight)
    live = jnp.concatenate([count[:, j : j + 1] for j in range(blocks)], axis=0)
    ranks = lax.broadcasted_iota(jnp.int32, (blocks, matches), 1)
    spots = lax.broadcasted_iota(jnp.int32, (blocks, LANES), 1)
    masked = jnp.where(ranks < live, weight, 0.0)
    share = masked / jnp.sum(masked, axis=1, keepdims=True)
    column = peer * slots + slot
    total = jnp.zeros_like(share)
    again = jnp.zeros_like(share)
    for k in range(matches):
        same = column == column[:, k : k + 1]
        total = total + jnp.where(same, share[:, k : k + 1], 0.0)
        again = again + jnp.where(jnp.logical_and(same, ranks > k), 1.0, 0.0)
    coef = jnp.where(again > 0.0, 0.0, total.astype(BF16).astype(F32))
    chosen = jnp.zeros_like(column)
    for q in range(peers):
        for k in range(slots):
            named = asked[0, k : k + 1, q : q + 1]
            chosen = chosen + jnp.where(column == q * slots + k, named, 0)
    place = peer * blocks + chosen
    line = jnp.zeros((blocks, LANES), F32)
    for k in range(matches):
        line = line + jnp.where(spots == place[:, k : k + 1], coef[:, k : k + 1], 0.0)
    high = line.astype(BF16).astype(F32)
    rows[...] = jnp.zeros_like(rows)
    rows[:blocks, :] = high
    rows[blocks : 2 * blocks, :] = line - high
    table[...] = rows[...].astype(BF16)
    for p in range(peers):
        pltpu.make_async_copy(table, out.at[p, pl.ds(pixels, TABLE_ROWS), :], extra.at[p]).start()
    for i in range(STEPS):
        at = pl.ds(i * step, step)
        pltpu.make_async_copy(tile.at[:, at, :], held.at[:, at, :], come.at[i]).wait()
        into = pl.ds(i * step * blocks, step * blocks)
        for p in range(peers):
            lanes = slice(p * LANES, (p + 1) * LANES)
            parts = [halves(held[j, at, lanes].astype(F32)) for j in range(blocks)]
            made[p, into, :] = weave(parts).astype(BF16)
        pltpu.make_async_copy(made.at[:, into, :], out.at[:, into, :], go.at[i]).start()
    for i in range(STEPS):
        into = pl.ds(i * step * blocks, step * blocks)
        pltpu.make_async_copy(made.at[:, into, :], out.at[:, into, :], go.at[i]).wait()
    for p in range(peers):
        pltpu.make_async_copy(table, out.at[p, pl.ds(pixels, TABLE_ROWS), :], extra.at[p]).wait()


def spread(tile, blocks, peers, peer, slot, count, weight, wanted):
    pixels, atoms = tile.shape
    shaped = tile.reshape(blocks, pixels // blocks, atoms)
    inputs = (wanted.transpose(0, 2, 1), peer, slot, count.T, weight, shaped)
    inputs = tuple(pltpu.with_memory_space_constraint(a, pltpu.HBM) for a in inputs)
    return pl.pallas_call(
        spread_kernel,
        in_specs=[pl.BlockSpec(memory_space=pltpu.HBM)] * len(inputs),
        out_specs=pl.BlockSpec(memory_space=pltpu.HBM),
        out_shape=pltpu.HBM((peers, pixels + TABLE_ROWS, LANES), tile.dtype),
        scratch_shapes=[
            pltpu.VMEM(shaped.shape, tile.dtype),
            pltpu.VMEM((peers, pixels, LANES), tile.dtype),
            *(pltpu.VMEM(a.shape, a.dtype) for a in inputs[:-1]),
            pltpu.VMEM((TABLE_ROWS, LANES), F32),
            pltpu.VMEM((TABLE_ROWS, LANES), BF16),
            pltpu.SemaphoreType.DMA((len(inputs) - 1,)),
            pltpu.SemaphoreType.DMA((STEPS,)),
            pltpu.SemaphoreType.DMA((STEPS,)),
            pltpu.SemaphoreType.DMA((peers,)),
        ],
        compiler_params=pltpu.CompilerParams(vmem_limit_bytes=16 * MIB),
        cost_estimate=cost(pixels * atoms, 4 * pixels * atoms),
        name="spread",
    )(*inputs)


def inverse_kernel(lib_ref, inv_ref):
    size = lib_ref.shape[0]
    lib = lib_ref[...]
    rows = lax.broadcasted_iota(jnp.int32, (size, size), 0)
    cols = lax.broadcasted_iota(jnp.int32, (size, size), 1)
    eye = (rows == cols).astype(F32)
    gram = times_transposed(lib, lib) + MU * eye
    bound = jnp.max(jnp.sum(jnp.abs(gram), axis=1, keepdims=True))
    inv_ref[...] = eye * (2.0 / (1.0 + bound))

    def exact(a, b):
        return jnp.dot(a, b, precision=lax.Precision.HIGHEST, preferred_element_type=F32)

    def unfinished(state):
        count, worst = state
        return jnp.logical_and(count < 22, worst > 1e-4)

    def improve(state):
        count, _ = state
        x = inv_ref[...]
        rest = eye - exact(gram, x)
        inv_ref[...] = x + exact(x, rest)
        return count + 1, jnp.max(jnp.sum(jnp.abs(rest), axis=1, keepdims=True))

    lax.while_loop(unfinished, improve, (jnp.int32(0), jnp.float32(1.0)))


def gram_inverse(lib):
    size = lib.shape[0]
    return pl.pallas_call(
        inverse_kernel,
        out_shape=jax.ShapeDtypeStruct((size, size), F32),
        cost_estimate=cost(10 * 12 * size**3, 4 * size * size),
        compiler_params=pltpu.CompilerParams(vmem_limit_bytes=63 * MIB),
        name="inverse",
    )(lib)


def solve_kernel(first, *refs):
    if first:
        obs, lib, inv, thr, z, up, down, left, right, parts, primal = refs[:11]
        padded, base, low, back = refs[11:]
    else:
        obs, lib, inv, thr, z, up, down, left, right, old_parts, old_primal, code, parts = refs[:13]
        padded, base, low, back, mix = refs[13:]
    i = pl.program_id(0)
    row = up.shape[0]
    block = obs.shape[0]
    peers = padded.shape[0]
    pixels = padded.shape[1] - 2 * row

    @pl.when(i == 0)
    def _():
        for p in range(peers):
            lanes = slice(p * LANES, (p + 1) * LANES)
            padded[p, :row, :] = up[:, lanes]
            padded[p, row + pixels :, :] = down[:, lanes]
            if first:
                padded[p, row : row + pixels, :] = z[:, lanes]

        def natural(p, carry):
            for k in range(STEPS):
                at = slice(k * pixels // STEPS, (k + 1) * pixels // STEPS)
                for j, rows in enumerate(unweave(z[p, at, :].astype(F32))):
                    to = j * block + k * block // STEPS
                    rows = rows.reshape(-1, LANES)
                    padded[p, row + to : row + to + rows.shape[0], :] = rows.astype(BF16)
                for j, rows in enumerate(unweave(decode_fixed(code[p, at, :]))):
                    to = j * block + k * block // STEPS
                    rows = rows.reshape(-1, LANES)
                    mix[p, to : to + rows.shape[0], :] = (GAMMA / TOTAL) * rows
            return carry

        if not first:
            lax.fori_loop(0, peers, natural, 0)

    at = pl.multiple_of(i * block, block)
    base[...] = jnp.dot(obs[...], lib[...], preferred_element_type=F32)
    for p in range(peers):
        lanes = slice(p * LANES, (p + 1) * LANES)
        value = base[:, lanes] + MU * padded[p, pl.ds(at + row, block), :].astype(F32)
        if not first:
            fresh = jnp.maximum(old_parts[:, lanes] + mix[p, pl.ds(at, block), :], 0.0)
            value = value + MU * (fresh - old_primal[:, lanes])
        low[:, lanes] = value.astype(BF16)
    small = times_transposed(low[...], lib[...])
    solved = jnp.dot(
        small, inv[...], precision=lax.Precision.HIGHEST, preferred_element_type=F32
    )
    back[...] = jnp.dot(solved.astype(BF16), lib[...], preferred_element_type=F32)
    place = lax.broadcasted_iota(jnp.int32, (block, LANES), 0) % row
    for p in range(peers):
        lanes = slice(p * LANES, (p + 1) * LANES)
        here = padded[p, pl.ds(at + row, block), :].astype(F32)
        above = padded[p, pl.ds(at, block), :].astype(F32)
        below = padded[p, pl.ds(at + 2 * row, block), :].astype(F32)

        def edge(halo):
            return jnp.concatenate(
                [
                    jnp.broadcast_to(halo[0, k : k + 1, lanes], (row, LANES))
                    for k in range(block // row)
                ],
                axis=0,
            )

        before = jnp.where(place == 0, edge(left), pltpu.roll(here, 1, 0))
        after = jnp.where(place == row - 1, edge(right), pltpu.roll(here, block - 1, 0))
        spatial = 0.25 * (above + below + before + after)
        unmixed = (base[:, lanes] + MU * here - back[:, lanes]) / MU
        if first:
            primal[:, lanes] = unmixed
        parts[:, lanes] = (unmixed + ETA * spatial) * (1.0 / TOTAL) - thr[:, lanes]


def solve(first, obs, lib, inv, thr, z, halos, carried=()):
    pixels = obs.shape[0]
    atoms = lib.shape[1]
    peers = atoms // LANES
    up, down, left, right = halos
    row = up.shape[0]
    block = BLOCK_ROWS * row
    steps = pixels // block
    whole = lambda a: pl.BlockSpec(a.shape, lambda i, n=a.ndim: (0,) * n)
    tile = pl.BlockSpec((block, atoms), lambda i: (i, 0))
    side = pl.BlockSpec((1, BLOCK_ROWS, atoms), lambda i: (i, 0, 0))
    full = jax.ShapeDtypeStruct((pixels, atoms), F32)
    return pl.pallas_call(
        functools.partial(solve_kernel, first),
        grid=(steps,),
        in_specs=[
            pl.BlockSpec((block, obs.shape[1]), lambda i: (i, 0)),
            whole(lib), whole(inv), whole(thr), whole(z), whole(up), whole(down), side, side,
        ]
        + ([] if first else [tile, tile, whole(carried[2])]),
        out_specs=[tile, tile] if first else tile,
        out_shape=[full, full] if first else full,
        scratch_shapes=[
            pltpu.VMEM((peers, pixels + 2 * row, LANES), BF16),
            pltpu.VMEM((block, atoms), F32),
            pltpu.VMEM((block, atoms), BF16),
            pltpu.VMEM((block, atoms), F32),
        ]
        + ([] if first else [pltpu.VMEM((peers, pixels, LANES), F32)]),
        cost_estimate=cost(6 * pixels * atoms * BANDS_PAD, 16 * pixels * atoms),
        compiler_params=pltpu.CompilerParams(vmem_limit_bytes=63 * MIB),
        name="solve_first" if first else "solve_second",
    )(obs, lib, inv, thr, z, up, down, left, right, *carried)


def weights_of(tables):
    size, spots = tables.shape
    rows = lax.broadcasted_iota(jnp.int32, (2 * size, size), 0)
    cols = lax.broadcasted_iota(jnp.int32, (2 * size, size), 1)
    inner = rows % size
    line = inner // 16 * 16 + inner % 16 // 4 + BLOCKS * (rows // size)
    pick = jnp.where(cols == line, 1.0, 0.0).astype(BF16)
    lines = jnp.dot(pick, tables, preferred_element_type=F32).astype(BF16)
    spot = lax.broadcasted_iota(jnp.int32, (spots, size), 0)
    col = lax.broadcasted_iota(jnp.int32, (spots, size), 1)
    widen = jnp.where(spot == col // 4, 1.0, 0.0).astype(BF16)
    wide = jnp.dot(lines, widen, preferred_element_type=F32)
    return jnp.where(rows % 4 == cols % 4, wide, 0.0).astype(BF16)


def mix_steps(encode, weights, z, out, made, go):
    peers, pixels, _ = made.shape
    size = peers * 16
    step = pixels // STEPS

    def rows_of(i):
        return pl.ds(pl.multiple_of(i * step, step), step)

    def one(i, carry):
        for k in range(0, step, 32):
            at = i * step + k
            tiles = [
                z[:, pl.ds(pl.multiple_of(at + d, 16), 16), :].reshape(size, LANES) for d in (0, 16)
            ]
            both = jnp.dot(
                weights[...], jnp.concatenate(tiles, axis=1), preferred_element_type=F32
            )
            coded = encode(both[:size] + both[size:])
            for d in (0, 1):
                made[:, pl.ds(pl.multiple_of(at + 16 * d, 16), 16), :] = coded[
                    :, d * LANES : (d + 1) * LANES
                ].reshape(peers, 16, LANES)
        rows = rows_of(i)
        pltpu.make_async_copy(made.at[:, rows, :], out.at[:, rows, :], go.at[i]).start()
        return carry

    lax.fori_loop(0, STEPS, one, 0)
    for i in range(STEPS):
        rows = pl.ds(i * step, step)
        pltpu.make_async_copy(made.at[:, rows, :], out.at[:, rows, :], go.at[i]).wait()


def mix_first_kernel(encode, z, out, table, made, weights, go, kept):
    pixels = made.shape[1]
    weights[...] = weights_of(z[:, pixels:, :].reshape(-1, LANES))
    keep = pltpu.make_async_copy(weights, table, kept)
    keep.start()
    mix_steps(encode, weights, z, out, made, go)
    keep.wait()


def mix_second_kernel(encode, weights, z, out, made, go):
    mix_steps(encode, weights, z, out, made, go)


def mix(encode, dtype, z, weights=None):
    peers = z.shape[0]
    pixels = z.shape[1] // LANES * LANES
    size = peers * 16
    hbm = pl.BlockSpec(memory_space=pltpu.HBM)
    vmem = pl.BlockSpec(memory_space=pltpu.VMEM)
    shape = pltpu.HBM((peers, pixels, LANES), dtype)
    made = pltpu.VMEM((peers, pixels, LANES), dtype)
    go = pltpu.SemaphoreType.DMA((STEPS,))
    first = weights is None
    return pl.pallas_call(
        functools.partial(mix_first_kernel if first else mix_second_kernel, encode),
        in_specs=[vmem] if first else [vmem, vmem],
        out_specs=[hbm, hbm] if first else hbm,
        out_shape=[shape, pltpu.HBM((2 * size, size), BF16)] if first else shape,
        scratch_shapes=[made, pltpu.VMEM((2 * size, size), BF16), go, pltpu.SemaphoreType.DMA]
        if first
        else [made, go],
        compiler_params=pltpu.CompilerParams(vmem_limit_bytes=48 * MIB),
        cost_estimate=cost(4 * size * pixels // 16 * LANES * size, 4 * peers * pixels * LANES),
        name="mix",
    )(*(() if first else (weights,)), z)


def fresh_kernel(
    parts, mixed, out, top_at, bottom_at, left_at, right_at,
    held, code, made, top, bottom, side, left, right, come, came, go, gone,
):
    blocks, block, _ = held.shape
    peers = made.shape[0]
    step = block // STEPS
    row = top.shape[0]
    reads, writes = [], []
    for i in range(STEPS):
        at = pl.ds(i * step, step)
        woven = pl.ds(i * step * blocks, step * blocks)
        reads.append(
            (
                pltpu.make_async_copy(parts.at[:, at, :], held.at[:, at, :], come.at[i]),
                pltpu.make_async_copy(mixed.at[:, woven, :], code.at[:, woven, :], came.at[i]),
            )
        )
        writes.append(pltpu.make_async_copy(made.at[:, woven, :], out.at[:, woven, :], go.at[i]))
    edges = ((top, top_at), (bottom, bottom_at), (left, left_at), (right, right_at))
    edges = [pltpu.make_async_copy(a, b, gone.at[k]) for k, (a, b) in enumerate(edges)]
    for pair in reads[:AHEAD]:
        for copy in pair:
            copy.start()
    for i in range(STEPS):
        for copy in reads[i]:
            copy.wait()
        if i + AHEAD < STEPS:
            for copy in reads[i + AHEAD]:
                copy.start()
        first = i * step
        at = slice(first, first + step)
        woven = slice(first * blocks, (first + step) * blocks)
        for p in range(peers):
            lanes = slice(p * LANES, (p + 1) * LANES)
            sums = unweave(decode_fixed(code[p, woven, :]))
            values = [
                jnp.maximum(halves(held[j, at, lanes]) + (GAMMA / TOTAL) * sums[j], 0.0)
                for j in range(blocks)
            ]
            made[p, woven, :] = weave(values).astype(BF16)
            if first < row:
                top[at, lanes] = values[0].reshape(step, LANES).astype(BF16)
            if first >= block - row:
                into = slice(first - block + row, first - block + row + step)
                bottom[into, lanes] = values[-1].reshape(step, LANES).astype(BF16)
            for j in range(blocks):
                line = j * BLOCK_ROWS + first // row
                if first % row == 0:
                    side[0, line : line + 1, lanes] = values[j][0, :1, :]
                if (first + step) % row == 0:
                    side[1, line : line + 1, lanes] = values[j][-1, 7:, :]
        writes[i].start()
    left[...] = side[0].astype(BF16)
    right[...] = side[1].astype(BF16)
    for copy in edges:
        copy.start()
    for copy in edges + writes:
        copy.wait()


def fresh_pieces(parts, mixed, tile_rows, tile_cols):
    peers, pixels, _ = mixed.shape
    atoms = parts.shape[1]
    hbm = pl.BlockSpec(memory_space=pltpu.HBM)
    shaped = parts.reshape(BLOCKS, pixels // BLOCKS, atoms)
    ends = ((tile_cols, atoms), (tile_cols, atoms), (tile_rows, atoms), (tile_rows, atoms))
    return pl.pallas_call(
        fresh_kernel,
        in_specs=[hbm, hbm],
        out_specs=[hbm] * 5,
        out_shape=[pltpu.HBM((peers, pixels, LANES), BF16)] + [pltpu.HBM(a, BF16) for a in ends],
        scratch_shapes=[
            pltpu.VMEM(shaped.shape, F32),
            pltpu.VMEM((peers, pixels, LANES), mixed.dtype),
            pltpu.VMEM((peers, pixels, LANES), BF16),
            pltpu.VMEM(ends[0], BF16),
            pltpu.VMEM(ends[1], BF16),
            pltpu.VMEM((2, tile_rows, atoms), F32),
            pltpu.VMEM(ends[2], BF16),
            pltpu.VMEM(ends[3], BF16),
            pltpu.SemaphoreType.DMA((STEPS,)),
            pltpu.SemaphoreType.DMA((STEPS,)),
            pltpu.SemaphoreType.DMA((STEPS,)),
            pltpu.SemaphoreType.DMA((4,)),
        ],
        compiler_params=pltpu.CompilerParams(vmem_limit_bytes=63 * MIB),
        cost_estimate=cost(4 * pixels * atoms, 8 * pixels * atoms),
        name="fresh",
    )(shaped, mixed)


def final_kernel(
    parts, mixed, obs, turned, out, misfit,
    held, code, made, rest, seen, spectra, come, came, go, went, side,
):
    blocks, block, atoms = held.shape
    step = block // STEPS
    wide = WIDE * step
    bands = rest.shape[2]
    reads, writes = [], []
    for i in range(STEPS):
        at = pl.ds(i * step, step)
        woven = pl.ds(i * step * blocks, step * blocks)
        reads.append(
            (
                pltpu.make_async_copy(parts.at[:, at, :], held.at[:, at, :], come.at[i]),
                pltpu.make_async_copy(mixed.at[:, woven, :], code.at[:, woven, :], came.at[i]),
            )
        )
        writes.append(pltpu.make_async_copy(made.at[:, at, :], out.at[:, at, :], go.at[i]))
    others = (
        pltpu.make_async_copy(turned, spectra, side.at[0]),
        pltpu.make_async_copy(obs, seen, side.at[1]),
    )
    for i, pair in enumerate(reads[:AHEAD]):
        for copy in pair:
            copy.start()
        if i == 0:
            for copy in others:
                copy.start()
    for i in range(STEPS):
        for copy in reads[i]:
            copy.wait()
        if i + AHEAD < STEPS:
            for copy in reads[i + AHEAD]:
                copy.start()
        at = slice(i * step, (i + 1) * step)
        woven = slice(i * step * blocks, (i + 1) * step * blocks)
        for p in range(mixed.shape[0]):
            lanes = slice(p * LANES, (p + 1) * LANES)
            sums = unweave(decode_float(code[p, woven, :]))
            for j in range(blocks):
                value = halves(held[j, at, lanes]) + (GAMMA / TOTAL) * sums[j]
                made[j, at, lanes] = jnp.maximum(value, 0.0).reshape(step, LANES).astype(BF16)
        writes[i].start()
        if i == 0:
            for copy in others:
                copy.wait()
        if (i + 1) % WIDE == 0:
            k = i // WIDE
            rows = pl.ds(k * wide, wide)
            rebuilt = jnp.dot(
                made[:, k * wide : (k + 1) * wide, :].reshape(blocks * wide, atoms),
                spectra[...],
                preferred_element_type=F32,
            )
            for j in range(blocks):
                real = seen[j, k * wide : (k + 1) * wide, :].astype(F32)
                less = real - rebuilt[j * wide : (j + 1) * wide]
                rest[j, k * wide : (k + 1) * wide, :] = less[:, :bands]
            writes.append(
                pltpu.make_async_copy(rest.at[:, rows, :], misfit.at[:, rows, :], went.at[k])
            )
            writes[-1].start()
    for copy in writes:
        copy.wait()


def final(parts, mixed, obs, turned, bands):
    peers, pixels, _ = mixed.shape
    atoms = parts.shape[1]
    by_block = lambda a: a.reshape(BLOCKS, pixels // BLOCKS, a.shape[1])
    parts, obs = by_block(parts), by_block(obs)
    hbm = pl.BlockSpec(memory_space=pltpu.HBM)
    left = (BLOCKS, pixels // BLOCKS, bands)
    return pl.pallas_call(
        final_kernel,
        in_specs=[hbm, hbm, hbm, hbm],
        out_specs=[hbm, hbm],
        out_shape=[pltpu.HBM(parts.shape, BF16), pltpu.HBM(left, F32)],
        scratch_shapes=[
            pltpu.VMEM(parts.shape, F32),
            pltpu.VMEM((peers, pixels, LANES), mixed.dtype),
            pltpu.VMEM(parts.shape, BF16),
            pltpu.VMEM(left, F32),
            pltpu.VMEM(obs.shape, obs.dtype),
            pltpu.VMEM(turned.shape, turned.dtype),
            pltpu.SemaphoreType.DMA((STEPS,)),
            pltpu.SemaphoreType.DMA((STEPS,)),
            pltpu.SemaphoreType.DMA((STEPS,)),
            pltpu.SemaphoreType.DMA((STEPS // WIDE,)),
            pltpu.SemaphoreType.DMA((2,)),
        ],
        compiler_params=pltpu.CompilerParams(vmem_limit_bytes=63 * MIB),
        cost_estimate=cost(2 * pixels * atoms * BANDS_PAD, 8 * pixels * atoms),
        name="final",
    )(parts, mixed, obs, turned)


def shifted(array, axis, up):
    peers = lax.axis_size(axis)
    pairs = [(k, k + 1) for k in range(peers - 1)]
    return lax.ppermute(array, axis, pairs if up else [(b, a) for a, b in pairs])


def exchanged(pieces):
    return lax.all_to_all(pieces, "col", 0, 0, tiled=True)


def halos_of(top, bottom, left, right):
    up = shifted(bottom, "row", True)
    down = shifted(top, "row", False)
    before = shifted(right, "col", True)
    after = shifted(left, "col", False)
    by_block = lambda a: a.astype(F32).reshape(BLOCKS, BLOCK_ROWS, -1)
    return up, down, by_block(before), by_block(after)


def local(
    observed, library, warm, match_peer, match_slot, match_count, match_weight, wanted, threshold
):
    tile_rows, tile_cols, atoms = warm.shape
    bands = library.shape[0]
    pixels = tile_rows * tile_cols
    peers = lax.axis_size("col")
    flat = warm.reshape(pixels, atoms)

    pieces = spread(
        flat, BLOCKS, peers,
        match_peer, match_slot, match_count, match_weight, wanted,
    )
    strip = exchanged(pieces)
    halos = halos_of(warm[0], warm[-1], warm[:, 0], warm[:, -1])
    lib = jnp.pad(library, ((0, BANDS_PAD - bands), (0, 0)))
    obs = jnp.pad(observed.reshape(pixels, bands), ((0, 0), (0, BANDS_PAD - bands)))
    inv = gram_inverse(lib)
    thr = threshold[None, :]

    sums, weights = mix(encode_fixed, jnp.int16, strip)
    mixed = exchanged(sums)
    parts, primal = solve(True, obs, lib, inv, thr, flat, halos)
    pieces, *edges = fresh_pieces(parts, mixed, tile_rows, tile_cols)
    strip = exchanged(pieces)
    halos = halos_of(*edges)
    sums = mix(encode_float, BF16, strip, weights)
    mixed_again = exchanged(sums)
    parts = solve(False, obs, lib, inv, thr, pieces, halos, (parts, primal, mixed))
    abundance, misfit = final(parts, mixed_again, obs, lib.T, bands)
    return (
        abundance.reshape(tile_rows, tile_cols, atoms),
        misfit.reshape(tile_rows, tile_cols, bands),
    )


def solution(mesh):
    return jax.shard_map(
        local,
        mesh=mesh,
        in_specs=(
            P("row", "col", None),
            P(),
            P("row", "col", None),
            P("row", "col", None),
            P("row", "col", None),
            P("row", "col"),
            P("row", "col", None),
            P("row", "col", None),
            P(),
        ),
        out_specs=(P("row", "col", None), P("row", "col", None)),
        check_vma=False,
    )
```

```python
import functools

import jax
import jax.numpy as jnp
from jax import lax
from jax.experimental import pallas as pl
from jax.experimental.pallas import tpu as pltpu
from jax.sharding import PartitionSpec as P


BLOCKS = 4
MU = 1.0
GAMMA = 0.6
ETA = 0.3
TOTAL = 1.0 + GAMMA + ETA
LANES = 128
BANDS_PAD = 192
CODE_SCALE = 64000.0
CODE_SHIFT = 32768.0
SLOPE = 4096.0
BEND = 0.125
STEPS = 8
AHEAD = 5
WIDE = 2
TABLE_ROWS = 16
MIB = 1024 * 1024

F32 = jnp.float32
BF16 = jnp.bfloat16


def cost(flops, moved):
    return pl.CostEstimate(flops=flops, bytes_accessed=moved, transcendentals=0)


def times_transposed(left, right):
    return lax.dot_general(
        left, right, (((1,), (1,)), ((), ())), preferred_element_type=F32
    )


def encode_fixed(value):
    return jnp.round(value * CODE_SCALE - CODE_SHIFT).astype(jnp.int32).astype(jnp.int16)


def decode_fixed(code):
    return (code.astype(jnp.int32).astype(F32) + CODE_SHIFT) * (1.0 / CODE_SCALE)


def encode_any(value):
    code = value * (SLOPE / (1.0 + BEND * jnp.abs(value)))
    return jnp.round(code).astype(jnp.int32).astype(jnp.int16)


def decode_any(code):
    real = code.astype(jnp.int32).astype(F32)
    return real / (SLOPE - BEND * jnp.abs(real))


def encode_positive(value):
    code = value * (2.0 * SLOPE / (1.0 + BEND * value)) - CODE_SHIFT
    return jnp.round(code).astype(jnp.int32).astype(jnp.int16)


def decode_positive(code):
    real = code.astype(jnp.int32).astype(F32) + CODE_SHIFT
    return real / (2.0 * SLOPE - BEND * real)


def swapped(a, b):
    low = lax.broadcasted_iota(jnp.int32, a.shape, 1) < 4
    first = jnp.where(low, a, pltpu.roll(b, 4, 1))
    second = jnp.where(low, pltpu.roll(a, 4, 1), b)
    return first, second


def weave(parts):
    f0, s0 = swapped(parts[0], parts[1])
    f1, s1 = swapped(parts[2], parts[3])
    tiles = [t[v] for v in range(f0.shape[0]) for t in (f0, f1, s0, s1)]
    return jnp.concatenate(tiles, axis=0)


def unweave(rows):
    tiles = rows.reshape(-1, 4, 8, LANES)
    b0, b1 = swapped(tiles[:, 0], tiles[:, 2])
    b2, b3 = swapped(tiles[:, 1], tiles[:, 3])
    return b0, b1, b2, b3


def halves(rows):
    return rows.reshape(-1, 8, LANES)


def spread_kernel(
    asked_at, peer_at, slot_at, count_at, weight_at, tile, out,
    held, made, asked, peer, slot, count, weight, rows, table, small, come, go, extra,
):
    blocks, block, _ = held.shape
    peers = made.shape[0]
    pixels = blocks * block
    step = block // STEPS
    for i in range(STEPS):
        at = pl.ds(i * step, step)
        pltpu.make_async_copy(tile.at[:, at, :], held.at[:, at, :], come.at[i]).start()
    tables = (
        (asked_at, asked), (peer_at, peer), (slot_at, slot), (count_at, count), (weight_at, weight),
    )
    for k, (source, target) in enumerate(tables):
        pltpu.make_async_copy(source, target, small.at[k]).start()
    for k, (source, target) in enumerate(tables):
        pltpu.make_async_copy(source, target, small.at[k]).wait()
    slots = asked.shape[1]
    matches = weight.shape[2]
    stacked = lambda ref: jnp.concatenate([ref[j] for j in range(blocks)], axis=0)
    peer, slot, weight = stacked(peer), stacked(slot), stacked(weight)
    live = jnp.concatenate([count[:, j : j + 1] for j in range(blocks)], axis=0)
    ranks = lax.broadcasted_iota(jnp.int32, (blocks, matches), 1)
    spots = lax.broadcasted_iota(jnp.int32, (blocks, LANES), 1)
    masked = jnp.where(ranks < live, weight, 0.0)
    share = masked / jnp.sum(masked, axis=1, keepdims=True)
    column = peer * slots + slot
    total = jnp.zeros_like(share)
    again = jnp.zeros_like(share)
    for k in range(matches):
        same = column == column[:, k : k + 1]
        total = total + jnp.where(same, share[:, k : k + 1], 0.0)
        again = again + jnp.where(jnp.logical_and(same, ranks > k), 1.0, 0.0)
    coef = jnp.where(again > 0.0, 0.0, total.astype(BF16).astype(F32))
    chosen = jnp.zeros_like(column)
    for q in range(peers):
        for k in range(slots):
            named = asked[0, k : k + 1, q : q + 1]
            chosen = chosen + jnp.where(column == q * slots + k, named, 0)
    place = peer * blocks + chosen
    line = jnp.zeros((blocks, LANES), F32)
    for k in range(matches):
        line = line + jnp.where(spots == place[:, k : k + 1], coef[:, k : k + 1], 0.0)
    high = line.astype(BF16).astype(F32)
    rows[...] = jnp.zeros_like(rows)
    rows[:blocks, :] = high
    rows[blocks : 2 * blocks, :] = line - high
    table[...] = rows[...].astype(BF16)
    for p in range(peers):
        pltpu.make_async_copy(table, out.at[p, pl.ds(pixels, TABLE_ROWS), :], extra.at[p]).start()
    for i in range(STEPS):
        at = pl.ds(i * step, step)
        pltpu.make_async_copy(tile.at[:, at, :], held.at[:, at, :], come.at[i]).wait()
        into = pl.ds(i * step * blocks, step * blocks)
        for p in range(peers):
            lanes = slice(p * LANES, (p + 1) * LANES)
            parts = [halves(held[j, at, lanes].astype(F32)) for j in range(blocks)]
            made[p, into, :] = weave(parts).astype(BF16)
        pltpu.make_async_copy(made.at[:, into, :], out.at[:, into, :], go.at[i]).start()
    for i in range(STEPS):
        into = pl.ds(i * step * blocks, step * blocks)
        pltpu.make_async_copy(made.at[:, into, :], out.at[:, into, :], go.at[i]).wait()
    for p in range(peers):
        pltpu.make_async_copy(table, out.at[p, pl.ds(pixels, TABLE_ROWS), :], extra.at[p]).wait()


def spread(tile, blocks, peers, peer, slot, count, weight, wanted):
    pixels, atoms = tile.shape
    shaped = tile.reshape(blocks, pixels // blocks, atoms)
    inputs = (wanted.transpose(0, 2, 1), peer, slot, count.T, weight, shaped)
    inputs = tuple(pltpu.with_memory_space_constraint(a, pltpu.HBM) for a in inputs)
    return pl.pallas_call(
        spread_kernel,
        in_specs=[pl.BlockSpec(memory_space=pltpu.HBM)] * len(inputs),
        out_specs=pl.BlockSpec(memory_space=pltpu.HBM),
        out_shape=pltpu.HBM((peers, pixels + TABLE_ROWS, LANES), tile.dtype),
        scratch_shapes=[
            pltpu.VMEM(shaped.shape, tile.dtype),
            pltpu.VMEM((peers, pixels, LANES), tile.dtype),
            *(pltpu.VMEM(a.shape, a.dtype) for a in inputs[:-1]),
            pltpu.VMEM((TABLE_ROWS, LANES), F32),
            pltpu.VMEM((TABLE_ROWS, LANES), BF16),
            pltpu.SemaphoreType.DMA((len(inputs) - 1,)),
            pltpu.SemaphoreType.DMA((STEPS,)),
            pltpu.SemaphoreType.DMA((STEPS,)),
            pltpu.SemaphoreType.DMA((peers,)),
        ],
        compiler_params=pltpu.CompilerParams(vmem_limit_bytes=16 * MIB),
        cost_estimate=cost(pixels * atoms, 4 * pixels * atoms),
        name="spread",
    )(*inputs)


def inverse_kernel(lib_ref, inv_ref):
    size = lib_ref.shape[0]
    lib = lib_ref[...]
    rows = lax.broadcasted_iota(jnp.int32, (size, size), 0)
    cols = lax.broadcasted_iota(jnp.int32, (size, size), 1)
    eye = (rows == cols).astype(F32)
    gram = times_transposed(lib, lib) + MU * eye
    bound = jnp.max(jnp.sum(jnp.abs(gram), axis=1, keepdims=True))
    inv_ref[...] = eye * (2.0 / (1.0 + bound))

    def exact(a, b):
        return jnp.dot(a, b, precision=lax.Precision.HIGHEST, preferred_element_type=F32)

    def unfinished(state):
        count, worst = state
        return jnp.logical_and(count < 22, worst > 1e-4)

    def improve(state):
        count, _ = state
        x = inv_ref[...]
        rest = eye - exact(gram, x)
        inv_ref[...] = x + exact(x, rest)
        return count + 1, jnp.max(jnp.sum(jnp.abs(rest), axis=1, keepdims=True))

    lax.while_loop(unfinished, improve, (jnp.int32(0), jnp.float32(1.0)))


def gram_inverse(lib):
    size = lib.shape[0]
    return pl.pallas_call(
        inverse_kernel,
        out_shape=jax.ShapeDtypeStruct((size, size), F32),
        cost_estimate=cost(10 * 12 * size**3, 4 * size * size),
        compiler_params=pltpu.CompilerParams(vmem_limit_bytes=63 * MIB),
        name="inverse",
    )(lib)


def solve_kernel(first, *refs):
    if first:
        obs, lib, inv, thr, z, parts, primal, lifted, base, low, back = refs
    else:
        obs, lib, inv, thr, old_parts, old_primal, code, parts, base, low, back, kept = refs
    blocks, row, bands = obs.shape
    count = blocks * row
    peers = base.shape[1] // LANES
    base[...] = jnp.dot(obs[...].reshape(count, bands), lib[...], preferred_element_type=F32)
    for p in range(peers):
        lanes = slice(p * LANES, (p + 1) * LANES)
        if first:
            value = base[:, lanes] + MU * z[:, :, lanes].astype(F32).reshape(count, LANES)
        else:
            sums = [a.reshape(row, LANES) for a in unweave(decode_fixed(code[p]))]
            mixed = (1.0 / TOTAL) * jnp.concatenate(sums, axis=0)
            fresh = jnp.maximum(old_parts[:, :, lanes].reshape(count, LANES) + mixed, 0.0)
            here = fresh.astype(BF16)
            kept[:, lanes] = here
            dual = fresh - old_primal[:, :, lanes].reshape(count, LANES)
            value = base[:, lanes] + MU * (here.astype(F32) + dual)
        low[:, lanes] = value.astype(BF16)
    small = times_transposed(low[...], lib[...])
    solved = jnp.dot(
        small, inv[...], precision=lax.Precision.HIGHEST, preferred_element_type=F32
    )
    back[...] = jnp.dot(solved.astype(BF16), lib[...], preferred_element_type=F32)
    for p in range(peers):
        lanes = slice(p * LANES, (p + 1) * LANES)
        if first:
            here = z[:, :, lanes].astype(F32).reshape(count, LANES)
        else:
            here = kept[:, lanes].astype(F32)
        unmixed = (base[:, lanes] + MU * here - back[:, lanes]) / MU
        made = unmixed * (1.0 / TOTAL) - thr[:, lanes]
        parts[:, :, lanes] = made.reshape(blocks, row, LANES)
        if first:
            primal[:, :, lanes] = unmixed.reshape(blocks, row, LANES)
            lifted[p] = encode_any(
                weave([halves(made[j * row : (j + 1) * row]) for j in range(blocks)])
            )


def solve(first, row, obs, lib, inv, thr, carried):
    pixels, bands = obs.shape
    atoms = lib.shape[1]
    peers = atoms // LANES
    block = pixels // BLOCKS
    count = BLOCKS * row
    whole = lambda a: pl.BlockSpec(a.shape, lambda i, n=a.ndim: (0,) * n)
    tile = pl.BlockSpec((BLOCKS, row, atoms), lambda i: (0, i, 0))
    piece = pl.BlockSpec((peers, count, LANES), lambda i: (0, i, 0))
    full = pltpu.HBM((BLOCKS, block, atoms), F32)
    sent = pltpu.HBM((peers, pixels, LANES), jnp.int16)
    return pl.pallas_call(
        functools.partial(solve_kernel, first),
        grid=(block // row,),
        in_specs=[
            pl.BlockSpec((BLOCKS, row, bands), lambda i: (0, i, 0)), whole(lib), whole(inv), whole(thr)
        ]
        + ([tile] if first else [tile, tile, piece]),
        out_specs=[tile, tile, piece] if first else tile,
        out_shape=[full, full, sent] if first else full,
        scratch_shapes=[
            pltpu.VMEM((count, atoms), F32),
            pltpu.VMEM((count, atoms), BF16),
            pltpu.VMEM((count, atoms), F32),
        ]
        + ([] if first else [pltpu.VMEM((count, atoms), BF16)]),
        compiler_params=pltpu.CompilerParams(vmem_limit_bytes=63 * MIB),
        cost_estimate=cost(6 * pixels * atoms * BANDS_PAD, 16 * pixels * atoms),
        name="solve_first" if first else "solve_second",
    )(obs.reshape(BLOCKS, block, bands), lib, inv, thr, *carried)


def weights_of(tables):
    size, spots = tables.shape
    rows = lax.broadcasted_iota(jnp.int32, (2 * size, size), 0)
    cols = lax.broadcasted_iota(jnp.int32, (2 * size, size), 1)
    inner = rows % size
    line = inner // 16 * 16 + inner % 16 // 4 + BLOCKS * (rows // size)
    pick = jnp.where(cols == line, 1.0, 0.0).astype(BF16)
    lines = jnp.dot(pick, tables, preferred_element_type=F32).astype(BF16)
    spot = lax.broadcasted_iota(jnp.int32, (spots, size), 0)
    col = lax.broadcasted_iota(jnp.int32, (spots, size), 1)
    widen = jnp.where(spot == col // 4, 1.0, 0.0).astype(BF16)
    wide = jnp.dot(lines, widen, preferred_element_type=F32)
    return jnp.where(rows % 4 == cols % 4, wide, 0.0).astype(BF16)


def beside(z, above, below, g, across):
    peers, pixels, _ = z.shape
    groups = pixels // 16

    def tile(ref, k):
        return ref[:, k * 16 : (k + 1) * 16, :].astype(F32).reshape(peers, 2, 8, LANES)

    def turned(a, by):
        return pltpu.roll(a.reshape(2 * peers, 8, LANES), by % 8, 1).reshape(a.shape)

    def part(ref, k):
        rows = ref[:, k * 8 : (k + 1) * 8, :].astype(F32)
        return pltpu.roll(rows, 4, 1).reshape(peers, 1, 8, LANES)

    here = tile(z, g)
    spot = lax.broadcasted_iota(jnp.int32, here.shape, 2)
    pixel = spot % 4
    none = jnp.zeros((1, 2, 8, LANES), F32)
    if g % across:
        before = tile(z, g - 1)
    else:
        before = jnp.concatenate([none, tile(z, g + across - 1)[:-1]], axis=0)
    if g % across < across - 1:
        after = tile(z, g + 1)
    else:
        after = jnp.concatenate([tile(z, g - across + 1)[1:], none], axis=0)
    left = jnp.where(pixel == 0, turned(before, -3), turned(here, 1))
    right = jnp.where(pixel == 3, turned(after, 3), turned(here, -1))
    if g >= across:
        up = tile(z, g - across)
    else:
        same = turned(tile(z, groups - across + g), 4)
        halo = part(above, g)
        up = jnp.where(spot < 4, jnp.concatenate([halo, same[:, :1]], axis=1), same)
    if g < groups - across:
        down = tile(z, g + across)
    else:
        same = turned(tile(z, g - groups + across), 4)
        halo = part(below, g - groups + across)
        down = jnp.where(spot < 4, same, jnp.concatenate([same[:, 1:], halo], axis=1))
    return (up + down + left + right).reshape(peers, 16, LANES)


def mix_kernel(
    encode, first, across, *refs
):
    if first:
        strip, above_at, below_at, out, table, z, above, below, made, tail, weights, come, go, other = refs
        quarters = []
    else:
        quarters, refs = refs[:4], refs[4:]
        above_at, below_at, table, out, z, above, below, made, weights, come, go, other = refs
    peers, pixels, _ = made.shape
    size = peers * 16
    step = pixels // STEPS
    copies = [
        pltpu.make_async_copy(above_at, above, come.at[0]),
        pltpu.make_async_copy(below_at, below, come.at[1]),
    ]
    for k, quarter in enumerate(quarters):
        rows = pl.ds(k * quarter.shape[1], quarter.shape[1])
        copies.append(pltpu.make_async_copy(quarter, z.at[:, rows, :], come.at[2 + k]))
    if first:
        copies.append(pltpu.make_async_copy(strip.at[:, pl.ds(0, pixels), :], z, come.at[2]))
        copies.append(
            pltpu.make_async_copy(strip.at[:, pl.ds(pixels, TABLE_ROWS), :], tail, other.at[0])
        )
    else:
        copies.append(pltpu.make_async_copy(table, weights, other.at[0]))
    for copy in copies:
        copy.start()
    for copy in copies:
        copy.wait()
    if first:
        weights[...] = weights_of(tail[...].reshape(-1, LANES))
        keep = pltpu.make_async_copy(weights, table, other.at[1])
        keep.start()
    writes = []
    for i in range(STEPS):
        rows = pl.ds(i * step, step)
        writes.append(pltpu.make_async_copy(made.at[:, rows, :], out.at[:, rows, :], go.at[i]))
        for at in range(i * step, (i + 1) * step, 32):
            tiles = [z[:, at + d : at + d + 16, :].reshape(size, LANES) for d in (0, 16)]
            both = jnp.dot(
                weights[...], jnp.concatenate(tiles, axis=1), preferred_element_type=F32
            )
            sums = both[:size] + both[size:]
            for d in (0, 1):
                averaged = sums[:, d * LANES : (d + 1) * LANES].reshape(peers, 16, LANES)
                around = beside(z, above, below, at // 16 + d, across)
                made[:, at + 16 * d : at + 16 * d + 16, :] = encode(
                    GAMMA * averaged + (0.25 * ETA) * around
                )
        writes[i].start()
    for copy in writes:
        copy.wait()
    if first:
        keep.wait()


def mix(encode, row, strip, above, below, weights=None):
    first = weights is None
    strips = (strip,) if first else strip
    peers, rows, _ = strips[0].shape
    pixels = rows - TABLE_ROWS if first else 4 * rows
    size = peers * 16
    hbm = pl.BlockSpec(memory_space=pltpu.HBM)
    shape = pltpu.HBM((peers, pixels, LANES), jnp.int16)
    edge = pltpu.VMEM(above.shape, BF16)
    return pl.pallas_call(
        functools.partial(mix_kernel, encode, first, row // 4),
        in_specs=[hbm] * (len(strips) + (2 if first else 3)),
        out_specs=[hbm, hbm] if first else hbm,
        out_shape=[shape, pltpu.HBM((2 * size, size), BF16)] if first else shape,
        scratch_shapes=[
            pltpu.VMEM((peers, pixels, LANES), BF16), edge, edge,
            pltpu.VMEM((peers, pixels, LANES), jnp.int16),
        ]
        + ([pltpu.VMEM((peers, TABLE_ROWS, LANES), BF16)] if first else [])
        + [
            pltpu.VMEM((2 * size, size), BF16),
            pltpu.SemaphoreType.DMA((2 + len(strips),)),
            pltpu.SemaphoreType.DMA((STEPS,)),
            pltpu.SemaphoreType.DMA((2,)),
        ],
        compiler_params=pltpu.CompilerParams(vmem_limit_bytes=63 * MIB),
        cost_estimate=cost(4 * size * pixels // 16 * LANES * size, 4 * peers * pixels * LANES),
        name="mix_first" if first else "mix_second",
    )(*strips, above, below, *(() if first else (weights,)))


def half_of(rows, h):
    return rows.reshape(-1, 2, 8, LANES)[:, h].reshape(-1, LANES)


def advance_kernel(strip_a, sums_a, strip_b, sums_b, out_a, out_b, *ends):
    for q in range(strip_a.shape[0]):
        for k, (strip, sums, out) in enumerate(
            ((strip_a, sums_a, out_a), (strip_b, sums_b, out_b))
        ):
            value = decode_any(strip[q]) + (1.0 / TOTAL) * decode_fixed(sums[q])
            value = jnp.maximum(value, 0.0)
            out[q] = value.astype(BF16)
            if ends:
                ends[k][q] = half_of(value, k).astype(BF16)


def advance(strip, sums, quarters, edge, with_ends):
    peers, pixels, _ = strip.shape
    step = 4
    specs = [pl.BlockSpec((step, edge, LANES), lambda i, k=k: (i, k, 0)) for k in quarters]
    whole = lambda n: pl.BlockSpec((step, n, LANES), lambda i: (i, 0, 0))
    sizes = [edge, edge] + ([edge // 2, edge // 2] if with_ends else [])
    return pl.pallas_call(
        advance_kernel,
        grid=(peers // step,),
        in_specs=[specs[0], specs[0], specs[1], specs[1]],
        out_specs=[whole(n) for n in sizes],
        out_shape=[pltpu.HBM((peers, n, LANES), BF16) for n in sizes],
        compiler_params=pltpu.CompilerParams(vmem_limit_bytes=63 * MIB),
        cost_estimate=cost(8 * peers * pixels * LANES, 3 * peers * pixels * LANES),
        name="advance_ends" if with_ends else "advance_middle",
    )(strip, sums, strip, sums)


def final_kernel(
    parts, mixed, obs, turned, out, misfit,
    held, code, made, rest, seen, spectra, come, came, go, went, side,
):
    blocks, block, atoms = held.shape
    step = block // STEPS
    wide = WIDE * step
    bands = rest.shape[2]
    reads, writes = [], []
    for i in range(STEPS):
        at = pl.ds(i * step, step)
        woven = pl.ds(i * step * blocks, step * blocks)
        reads.append(
            (
                pltpu.make_async_copy(parts.at[:, at, :], held.at[:, at, :], come.at[i]),
                pltpu.make_async_copy(mixed.at[:, woven, :], code.at[:, woven, :], came.at[i]),
            )
        )
        writes.append(pltpu.make_async_copy(made.at[:, at, :], out.at[:, at, :], go.at[i]))
    others = (
        pltpu.make_async_copy(turned, spectra, side.at[0]),
        pltpu.make_async_copy(obs, seen, side.at[1]),
    )
    for i, pair in enumerate(reads[:AHEAD]):
        for copy in pair:
            copy.start()
        if i == 0:
            for copy in others:
                copy.start()
    for i in range(STEPS):
        for copy in reads[i]:
            copy.wait()
        if i + AHEAD < STEPS:
            for copy in reads[i + AHEAD]:
                copy.start()
        at = slice(i * step, (i + 1) * step)
        woven = slice(i * step * blocks, (i + 1) * step * blocks)
        for p in range(mixed.shape[0]):
            lanes = slice(p * LANES, (p + 1) * LANES)
            sums = unweave(decode_positive(code[p, woven, :]))
            for j in range(blocks):
                value = halves(held[j, at, lanes]) + (1.0 / TOTAL) * sums[j]
                made[j, at, lanes] = jnp.maximum(value, 0.0).reshape(step, LANES).astype(BF16)
        writes[i].start()
        if i == 0:
            for copy in others:
                copy.wait()
        if (i + 1) % WIDE == 0:
            k = i // WIDE
            rows = pl.ds(k * wide, wide)
            rebuilt = jnp.dot(
                made[:, k * wide : (k + 1) * wide, :].reshape(blocks * wide, atoms),
                spectra[...],
                preferred_element_type=F32,
            )
            for j in range(blocks):
                real = seen[j, k * wide : (k + 1) * wide, :].astype(F32)
                less = real - rebuilt[j * wide : (j + 1) * wide]
                rest[j, k * wide : (k + 1) * wide, :] = less[:, :bands]
            writes.append(
                pltpu.make_async_copy(rest.at[:, rows, :], misfit.at[:, rows, :], went.at[k])
            )
            writes[-1].start()
    for copy in writes:
        copy.wait()


def final(parts, mixed, obs, turned, bands):
    peers, pixels, _ = mixed.shape
    atoms = parts.shape[2]
    obs = obs.reshape(BLOCKS, pixels // BLOCKS, obs.shape[1])
    hbm = pl.BlockSpec(memory_space=pltpu.HBM)
    left = (BLOCKS, pixels // BLOCKS, bands)
    return pl.pallas_call(
        final_kernel,
        in_specs=[hbm, hbm, hbm, hbm],
        out_specs=[hbm, hbm],
        out_shape=[pltpu.HBM(parts.shape, BF16), pltpu.HBM(left, F32)],
        scratch_shapes=[
            pltpu.VMEM(parts.shape, F32),
            pltpu.VMEM((peers, pixels, LANES), mixed.dtype),
            pltpu.VMEM(parts.shape, BF16),
            pltpu.VMEM(left, F32),
            pltpu.VMEM(obs.shape, obs.dtype),
            pltpu.VMEM(turned.shape, turned.dtype),
            pltpu.SemaphoreType.DMA((STEPS,)),
            pltpu.SemaphoreType.DMA((STEPS,)),
            pltpu.SemaphoreType.DMA((STEPS,)),
            pltpu.SemaphoreType.DMA((STEPS // WIDE,)),
            pltpu.SemaphoreType.DMA((2,)),
        ],
        compiler_params=pltpu.CompilerParams(vmem_limit_bytes=63 * MIB),
        cost_estimate=cost(2 * pixels * atoms * BANDS_PAD, 8 * pixels * atoms),
        name="final",
    )(parts, mixed, obs, turned)


def shifted(array, axis, up):
    peers = lax.axis_size(axis)
    pairs = [(k, k + 1) for k in range(peers - 1)]
    return lax.ppermute(array, axis, pairs if up else [(b, a) for a, b in pairs])


def exchanged(pieces):
    return lax.all_to_all(pieces, "col", 0, 0, tiled=True)


def strip_ends(strip, pixels, edge):
    tiles = strip[:, :pixels].reshape(strip.shape[0], pixels // 16, 2, 8, LANES)
    rows = lambda a: a.reshape(strip.shape[0], edge // 2, LANES)
    return rows(tiles[:, : edge // 16, 0]), rows(tiles[:, (pixels - edge) // 16 :, 1])


def strip_halos(first, last):
    above = shifted(last, "row", True)
    below = shifted(first, "row", False)
    return above, below


def local(
    observed, library, warm, match_peer, match_slot, match_count, match_weight, wanted, threshold
):
    tile_rows, tile_cols, atoms = warm.shape
    bands = library.shape[0]
    pixels = tile_rows * tile_cols
    peers = lax.axis_size("col")
    flat = warm.reshape(pixels, atoms)

    pieces = spread(
        flat, BLOCKS, peers,
        match_peer, match_slot, match_count, match_weight, wanted,
    )
    strip = exchanged(pieces)
    lib = jnp.pad(library, ((0, BANDS_PAD - bands), (0, 0)))
    obs = jnp.pad(observed.reshape(pixels, bands), ((0, 0), (0, BANDS_PAD - bands)))
    inv = gram_inverse(lib)
    thr = threshold[None, :]

    by_block = flat.reshape(BLOCKS, pixels // BLOCKS, atoms)
    parts, primal, lifted = solve(True, tile_cols, obs, lib, inv, thr, (by_block,))
    strip_parts = exchanged(lifted)
    edge = BLOCKS * tile_cols
    above, below = strip_halos(*strip_ends(strip, pixels, edge))
    sums, weights = mix(encode_fixed, tile_cols, strip, above, below)
    mixed = exchanged(sums)
    first, last, *ends = advance(strip_parts, sums, (0, 3), edge, True)
    above, below = strip_halos(*ends)
    middle = advance(strip_parts, sums, (1, 2), edge, False)
    strip = (first, *middle, last)
    sums = mix(encode_positive, tile_cols, strip, above, below, weights)
    mixed_again = exchanged(sums)
    parts = solve(False, tile_cols, obs, lib, inv, thr, (parts, primal, mixed))
    abundance, misfit = final(parts, mixed_again, obs, lib.T, bands)
    return (
        abundance.reshape(tile_rows, tile_cols, atoms),
        misfit.reshape(tile_rows, tile_cols, bands),
    )


def solution(mesh):
    return jax.shard_map(
        local,
        mesh=mesh,
        in_specs=(
            P("row", "col", None),
            P(),
            P("row", "col", None),
            P("row", "col", None),
            P("row", "col", None),
            P("row", "col"),
            P("row", "col", None),
            P("row", "col", None),
            P(),
        ),
        out_specs=(P("row", "col", None), P("row", "col", None)),
        check_vma=False,
    )
```

```python
import functools

import jax
import jax.numpy as jnp
from jax import lax
from jax.experimental import pallas as pl
from jax.experimental.pallas import tpu as pltpu
from jax.sharding import PartitionSpec as P


BLOCKS = 4
MU = 1.0
GAMMA = 0.6
ETA = 0.3
TOTAL = 1.0 + GAMMA + ETA
LANES = 128
BANDS_PAD = 192
CODE_SCALE = 64000.0
CODE_SHIFT = 32768.0
SLOPE = 4096.0
BEND = 0.125
STEPS = 8
AHEAD = 5
WIDE = 2
TABLE_ROWS = 8
MIB = 1024 * 1024

F32 = jnp.float32
BF16 = jnp.bfloat16


def cost(flops, moved):
    return pl.CostEstimate(flops=flops, bytes_accessed=moved, transcendentals=0)


def times_transposed(left, right):
    return lax.dot_general(
        left, right, (((1,), (1,)), ((), ())), preferred_element_type=F32
    )


def encode_fixed(value):
    return jnp.round(value * CODE_SCALE - CODE_SHIFT).astype(jnp.int32).astype(jnp.int16)


def decode_fixed(code):
    return (code.astype(jnp.int32).astype(F32) + CODE_SHIFT) * (1.0 / CODE_SCALE)


def encode_any(value):
    code = value * (SLOPE / (1.0 + BEND * jnp.abs(value)))
    return jnp.round(code).astype(jnp.int32).astype(jnp.int16)


def decode_any(code):
    real = code.astype(jnp.int32).astype(F32)
    return real / (SLOPE - BEND * jnp.abs(real))


def encode_positive(value):
    code = value * (2.0 * SLOPE / (1.0 + BEND * value)) - CODE_SHIFT
    return jnp.round(code).astype(jnp.int32).astype(jnp.int16)


def decode_positive(code):
    real = code.astype(jnp.int32).astype(F32) + CODE_SHIFT
    return real / (2.0 * SLOPE - BEND * real)


def swapped(a, b):
    low = lax.broadcasted_iota(jnp.int32, a.shape, 1) < 4
    first = jnp.where(low, a, pltpu.roll(b, 4, 1))
    second = jnp.where(low, pltpu.roll(a, 4, 1), b)
    return first, second


def weave(parts):
    f0, s0 = swapped(parts[0], parts[1])
    f1, s1 = swapped(parts[2], parts[3])
    tiles = [t[v] for v in range(f0.shape[0]) for t in (f0, f1, s0, s1)]
    return jnp.concatenate(tiles, axis=0)


def unweave(rows):
    tiles = rows.reshape(-1, 4, 8, LANES)
    b0, b1 = swapped(tiles[:, 0], tiles[:, 2])
    b2, b3 = swapped(tiles[:, 1], tiles[:, 3])
    return b0, b1, b2, b3


def halves(rows):
    return rows.reshape(-1, 8, LANES)


def spread_kernel(
    asked_at, peer_at, slot_at, count_at, weight_at, tile, out,
    held, made, asked, peer, slot, count, weight, rows, table, small, come, go, extra,
):
    blocks, block, _ = held.shape
    peers = made.shape[0]
    pixels = blocks * block
    step = block // STEPS
    for i in range(STEPS):
        at = pl.ds(i * step, step)
        pltpu.make_async_copy(tile.at[:, at, :], held.at[:, at, :], come.at[i]).start()
    tables = (
        (asked_at, asked), (peer_at, peer), (slot_at, slot), (count_at, count), (weight_at, weight),
    )
    for k, (source, target) in enumerate(tables):
        pltpu.make_async_copy(source, target, small.at[k]).start()
    for k, (source, target) in enumerate(tables):
        pltpu.make_async_copy(source, target, small.at[k]).wait()
    slots = asked.shape[1]
    matches = weight.shape[2]
    stacked = lambda ref: jnp.concatenate([ref[j] for j in range(blocks)], axis=0)
    peer, slot, weight = stacked(peer), stacked(slot), stacked(weight)
    live = jnp.concatenate([count[:, j : j + 1] for j in range(blocks)], axis=0)
    ranks = lax.broadcasted_iota(jnp.int32, (blocks, matches), 1)
    spots = lax.broadcasted_iota(jnp.int32, (blocks, LANES), 1)
    masked = jnp.where(ranks < live, weight, 0.0)
    share = masked / jnp.sum(masked, axis=1, keepdims=True)
    column = peer * slots + slot
    total = jnp.zeros_like(share)
    again = jnp.zeros_like(share)
    for k in range(matches):
        same = column == column[:, k : k + 1]
        total = total + jnp.where(same, share[:, k : k + 1], 0.0)
        again = again + jnp.where(jnp.logical_and(same, ranks > k), 1.0, 0.0)
    coef = jnp.where(again > 0.0, 0.0, total.astype(BF16).astype(F32))
    chosen = jnp.zeros_like(column)
    for q in range(peers):
        for k in range(slots):
            named = asked[0, k : k + 1, q : q + 1]
            chosen = chosen + jnp.where(column == q * slots + k, named, 0)
    place = peer * blocks + chosen
    line = jnp.zeros((blocks, LANES), F32)
    for k in range(matches):
        line = line + jnp.where(spots == place[:, k : k + 1], coef[:, k : k + 1], 0.0)
    high = line.astype(BF16).astype(F32)
    rows[...] = jnp.zeros_like(rows)
    rows[:blocks, :] = high
    rows[blocks : 2 * blocks, :] = line - high
    table[...] = rows[...].astype(BF16)
    for p in range(peers):
        pltpu.make_async_copy(table, out.at[p, pl.ds(pixels, TABLE_ROWS), :], extra.at[p]).start()
    for i in range(STEPS):
        at = pl.ds(i * step, step)
        pltpu.make_async_copy(tile.at[:, at, :], held.at[:, at, :], come.at[i]).wait()
        into = pl.ds(i * step * blocks, step * blocks)
        for p in range(peers):
            lanes = slice(p * LANES, (p + 1) * LANES)
            parts = [halves(held[j, at, lanes].astype(F32)) for j in range(blocks)]
            made[p, into, :] = weave(parts).astype(BF16)
        pltpu.make_async_copy(made.at[:, into, :], out.at[:, into, :], go.at[i]).start()
    for i in range(STEPS):
        into = pl.ds(i * step * blocks, step * blocks)
        pltpu.make_async_copy(made.at[:, into, :], out.at[:, into, :], go.at[i]).wait()
    for p in range(peers):
        pltpu.make_async_copy(table, out.at[p, pl.ds(pixels, TABLE_ROWS), :], extra.at[p]).wait()


def spread(tile, blocks, peers, peer, slot, count, weight, wanted):
    pixels, atoms = tile.shape
    shaped = tile.reshape(blocks, pixels // blocks, atoms)
    inputs = (wanted.transpose(0, 2, 1), peer, slot, count.T, weight, shaped)
    inputs = tuple(pltpu.with_memory_space_constraint(a, pltpu.HBM) for a in inputs)
    return pl.pallas_call(
        spread_kernel,
        in_specs=[pl.BlockSpec(memory_space=pltpu.HBM)] * len(inputs),
        out_specs=pl.BlockSpec(memory_space=pltpu.HBM),
        out_shape=pltpu.HBM((peers, pixels + TABLE_ROWS, LANES), tile.dtype),
        scratch_shapes=[
            pltpu.VMEM(shaped.shape, tile.dtype),
            pltpu.VMEM((peers, pixels, LANES), tile.dtype),
            *(pltpu.VMEM(a.shape, a.dtype) for a in inputs[:-1]),
            pltpu.VMEM((TABLE_ROWS, LANES), F32),
            pltpu.VMEM((TABLE_ROWS, LANES), BF16),
            pltpu.SemaphoreType.DMA((len(inputs) - 1,)),
            pltpu.SemaphoreType.DMA((STEPS,)),
            pltpu.SemaphoreType.DMA((STEPS,)),
            pltpu.SemaphoreType.DMA((peers,)),
        ],
        compiler_params=pltpu.CompilerParams(vmem_limit_bytes=16 * MIB),
        cost_estimate=cost(pixels * atoms, 4 * pixels * atoms),
        name="spread",
    )(*inputs)


def inverse_kernel(lib_ref, inv_ref):
    size = lib_ref.shape[0]
    lib = lib_ref[...]
    rows = lax.broadcasted_iota(jnp.int32, (size, size), 0)
    cols = lax.broadcasted_iota(jnp.int32, (size, size), 1)
    eye = (rows == cols).astype(F32)
    gram = times_transposed(lib, lib) + MU * eye
    bound = jnp.max(jnp.sum(jnp.abs(gram), axis=1, keepdims=True))
    inv_ref[...] = eye * (2.0 / (1.0 + bound))

    def exact(a, b):
        return jnp.dot(a, b, precision=lax.Precision.HIGHEST, preferred_element_type=F32)

    def unfinished(state):
        count, worst = state
        return jnp.logical_and(count < 22, worst > 1e-4)

    def improve(state):
        count, _ = state
        x = inv_ref[...]
        rest = eye - exact(gram, x)
        inv_ref[...] = x + exact(x, rest)
        return count + 1, jnp.max(jnp.sum(jnp.abs(rest), axis=1, keepdims=True))

    lax.while_loop(unfinished, improve, (jnp.int32(0), jnp.float32(1.0)))


def gram_inverse(lib):
    size = lib.shape[0]
    return pl.pallas_call(
        inverse_kernel,
        out_shape=jax.ShapeDtypeStruct((size, size), F32),
        cost_estimate=cost(10 * 12 * size**3, 4 * size * size),
        compiler_params=pltpu.CompilerParams(vmem_limit_bytes=63 * MIB),
        name="inverse",
    )(lib)


def solve_kernel(first, *refs):
    if first:
        obs, lib, inv, thr, z, parts, primal, lifted, base, low, back = refs
    else:
        obs, lib, inv, thr, old_parts, old_primal, code, parts, base, low, back, kept = refs
    blocks, row, bands = obs.shape
    count = blocks * row
    peers = base.shape[1] // LANES
    base[...] = jnp.dot(obs[...].reshape(count, bands), lib[...], preferred_element_type=F32)
    for p in range(peers):
        lanes = slice(p * LANES, (p + 1) * LANES)
        if first:
            value = base[:, lanes] + MU * z[:, :, lanes].astype(F32).reshape(count, LANES)
        else:
            sums = [a.reshape(row, LANES) for a in unweave(decode_fixed(code[p]))]
            mixed = (1.0 / TOTAL) * jnp.concatenate(sums, axis=0)
            fresh = jnp.maximum(old_parts[:, :, lanes].reshape(count, LANES) + mixed, 0.0)
            here = fresh.astype(BF16)
            kept[:, lanes] = here
            dual = fresh - old_primal[:, :, lanes].reshape(count, LANES)
            value = base[:, lanes] + MU * (here.astype(F32) + dual)
        low[:, lanes] = value.astype(BF16)
    small = times_transposed(low[...], lib[...])
    solved = jnp.dot(
        small, inv[...], precision=lax.Precision.HIGHEST, preferred_element_type=F32
    )
    back[...] = jnp.dot(solved.astype(BF16), lib[...], preferred_element_type=F32)
    for p in range(peers):
        lanes = slice(p * LANES, (p + 1) * LANES)
        if first:
            here = z[:, :, lanes].astype(F32).reshape(count, LANES)
        else:
            here = kept[:, lanes].astype(F32)
        unmixed = (base[:, lanes] + MU * here - back[:, lanes]) / MU
        made = unmixed * (1.0 / TOTAL) - thr[:, lanes]
        parts[:, :, lanes] = made.reshape(blocks, row, LANES)
        if first:
            primal[:, :, lanes] = unmixed.reshape(blocks, row, LANES)
            lifted[p] = encode_any(
                weave([halves(made[j * row : (j + 1) * row]) for j in range(blocks)])
            )


def solve(first, row, obs, lib, inv, thr, carried):
    pixels, bands = obs.shape
    atoms = lib.shape[1]
    peers = atoms // LANES
    block = pixels // BLOCKS
    count = BLOCKS * row
    whole = lambda a: pl.BlockSpec(a.shape, lambda i, n=a.ndim: (0,) * n)
    tile = pl.BlockSpec((BLOCKS, row, atoms), lambda i: (0, i, 0))
    piece = pl.BlockSpec((peers, count, LANES), lambda i: (0, i, 0))
    full = pltpu.HBM((BLOCKS, block, atoms), F32)
    sent = pltpu.HBM((peers, pixels, LANES), jnp.int16)
    return pl.pallas_call(
        functools.partial(solve_kernel, first),
        grid=(block // row,),
        in_specs=[
            pl.BlockSpec((BLOCKS, row, bands), lambda i: (0, i, 0)), whole(lib), whole(inv), whole(thr)
        ]
        + ([tile] if first else [tile, tile, piece]),
        out_specs=[tile, tile, piece] if first else tile,
        out_shape=[full, full, sent] if first else full,
        scratch_shapes=[
            pltpu.VMEM((count, atoms), F32),
            pltpu.VMEM((count, atoms), BF16),
            pltpu.VMEM((count, atoms), F32),
        ]
        + ([] if first else [pltpu.VMEM((count, atoms), BF16)]),
        compiler_params=pltpu.CompilerParams(vmem_limit_bytes=63 * MIB),
        cost_estimate=cost(6 * pixels * atoms * BANDS_PAD, 16 * pixels * atoms),
        name="solve_first" if first else "solve_second",
    )(obs.reshape(BLOCKS, block, bands), lib, inv, thr, *carried)


def weights_of(tables, size):
    lines, spots = tables.shape
    rows = lax.broadcasted_iota(jnp.int32, (2 * size, lines), 0)
    cols = lax.broadcasted_iota(jnp.int32, (2 * size, lines), 1)
    inner = rows % size
    line = inner // 16 * TABLE_ROWS + inner % 16 // 4 + BLOCKS * (rows // size)
    pick = jnp.where(cols == line, 1.0, 0.0).astype(BF16)
    lines = jnp.dot(pick, tables, preferred_element_type=F32).astype(BF16)
    spot = lax.broadcasted_iota(jnp.int32, (spots, size), 0)
    col = lax.broadcasted_iota(jnp.int32, (spots, size), 1)
    widen = jnp.where(spot == col // 4, 1.0, 0.0).astype(BF16)
    wide = jnp.dot(lines, widen, preferred_element_type=F32)
    rows = lax.broadcasted_iota(jnp.int32, (2 * size, size), 0)
    cols = lax.broadcasted_iota(jnp.int32, (2 * size, size), 1)
    return jnp.where(rows % 4 == cols % 4, wide, 0.0).astype(BF16)


def beside(z, above, below, g, across):
    peers, pixels, _ = z.shape
    groups = pixels // 16

    def tile(ref, k):
        return ref[:, k * 16 : (k + 1) * 16, :].astype(F32).reshape(peers, 2, 8, LANES)

    def turned(a, by):
        return pltpu.roll(a.reshape(2 * peers, 8, LANES), by % 8, 1).reshape(a.shape)

    def part(ref, k):
        rows = ref[:, k * 8 : (k + 1) * 8, :].astype(F32)
        return pltpu.roll(rows, 4, 1).reshape(peers, 1, 8, LANES)

    here = tile(z, g)
    spot = lax.broadcasted_iota(jnp.int32, here.shape, 2)
    pixel = spot % 4
    none = jnp.zeros((1, 2, 8, LANES), F32)
    if g % across:
        before = tile(z, g - 1)
    else:
        before = jnp.concatenate([none, tile(z, g + across - 1)[:-1]], axis=0)
    if g % across < across - 1:
        after = tile(z, g + 1)
    else:
        after = jnp.concatenate([tile(z, g - across + 1)[1:], none], axis=0)
    left = jnp.where(pixel == 0, turned(before, -3), turned(here, 1))
    right = jnp.where(pixel == 3, turned(after, 3), turned(here, -1))
    if g >= across:
        up = tile(z, g - across)
    else:
        same = turned(tile(z, groups - across + g), 4)
        halo = part(above, g)
        up = jnp.where(spot < 4, jnp.concatenate([halo, same[:, :1]], axis=1), same)
    if g < groups - across:
        down = tile(z, g + across)
    else:
        same = turned(tile(z, g - groups + across), 4)
        halo = part(below, g - groups + across)
        down = jnp.where(spot < 4, same, jnp.concatenate([same[:, 1:], halo], axis=1))
    return (up + down + left + right).reshape(peers, 16, LANES)


def mix_kernel(
    encode, first, across, *refs
):
    if first:
        strip, above_at, below_at, out, table, z, above, below, made, tail, weights, come, go, other = refs
        quarters = []
    else:
        quarters, refs = refs[:4], refs[4:]
        above_at, below_at, table, out, z, above, below, made, weights, come, go, other = refs
    peers, pixels, _ = made.shape
    size = peers * 16
    step = pixels // STEPS
    copies = [
        pltpu.make_async_copy(above_at, above, come.at[0]),
        pltpu.make_async_copy(below_at, below, come.at[1]),
    ]
    for k, quarter in enumerate(quarters):
        rows = pl.ds(k * quarter.shape[1], quarter.shape[1])
        copies.append(pltpu.make_async_copy(quarter, z.at[:, rows, :], come.at[2 + k]))
    if first:
        copies.append(pltpu.make_async_copy(strip.at[:, pl.ds(0, pixels), :], z, come.at[2]))
        copies.append(
            pltpu.make_async_copy(strip.at[:, pl.ds(pixels, TABLE_ROWS), :], tail, other.at[0])
        )
    else:
        copies.append(pltpu.make_async_copy(table, weights, other.at[0]))
    for copy in copies:
        copy.start()
    for copy in copies:
        copy.wait()
    if first:
        tables = tail[...].astype(F32).reshape(-1, LANES).astype(BF16)
        weights[...] = weights_of(tables, size)
        keep = pltpu.make_async_copy(weights, table, other.at[1])
        keep.start()
    writes = []
    for i in range(STEPS):
        rows = pl.ds(i * step, step)
        writes.append(pltpu.make_async_copy(made.at[:, rows, :], out.at[:, rows, :], go.at[i]))
        for at in range(i * step, (i + 1) * step, 32):
            tiles = [z[:, at + d : at + d + 16, :].reshape(size, LANES) for d in (0, 16)]
            both = jnp.dot(
                weights[...], jnp.concatenate(tiles, axis=1), preferred_element_type=F32
            )
            sums = both[:size] + both[size:]
            for d in (0, 1):
                averaged = sums[:, d * LANES : (d + 1) * LANES].reshape(peers, 16, LANES)
                around = beside(z, above, below, at // 16 + d, across)
                made[:, at + 16 * d : at + 16 * d + 16, :] = encode(
                    GAMMA * averaged + (0.25 * ETA) * around
                )
        writes[i].start()
    for copy in writes:
        copy.wait()
    if first:
        keep.wait()


def mix(encode, row, strip, above, below, weights=None):
    first = weights is None
    strips = (strip,) if first else strip
    peers, rows, _ = strips[0].shape
    pixels = rows - TABLE_ROWS if first else 4 * rows
    size = peers * 16
    hbm = pl.BlockSpec(memory_space=pltpu.HBM)
    shape = pltpu.HBM((peers, pixels, LANES), jnp.int16)
    edge = pltpu.VMEM(above.shape, BF16)
    return pl.pallas_call(
        functools.partial(mix_kernel, encode, first, row // 4),
        in_specs=[hbm] * (len(strips) + (2 if first else 3)),
        out_specs=[hbm, hbm] if first else hbm,
        out_shape=[shape, pltpu.HBM((2 * size, size), BF16)] if first else shape,
        scratch_shapes=[
            pltpu.VMEM((peers, pixels, LANES), BF16), edge, edge,
            pltpu.VMEM((peers, pixels, LANES), jnp.int16),
        ]
        + ([pltpu.VMEM((peers, TABLE_ROWS, LANES), BF16)] if first else [])
        + [
            pltpu.VMEM((2 * size, size), BF16),
            pltpu.SemaphoreType.DMA((2 + len(strips),)),
            pltpu.SemaphoreType.DMA((STEPS,)),
            pltpu.SemaphoreType.DMA((2,)),
        ],
        compiler_params=pltpu.CompilerParams(vmem_limit_bytes=63 * MIB),
        cost_estimate=cost(4 * size * pixels // 16 * LANES * size, 4 * peers * pixels * LANES),
        name="mix_first" if first else "mix_second",
    )(*strips, above, below, *(() if first else (weights,)))


def half_of(rows, h):
    return rows.reshape(-1, 2, 8, LANES)[:, h].reshape(-1, LANES)


def advance_kernel(strip_a, sums_a, strip_b, sums_b, out_a, out_b, *ends):
    for q in range(strip_a.shape[0]):
        for k, (strip, sums, out) in enumerate(
            ((strip_a, sums_a, out_a), (strip_b, sums_b, out_b))
        ):
            value = decode_any(strip[q]) + (1.0 / TOTAL) * decode_fixed(sums[q])
            value = jnp.maximum(value, 0.0)
            out[q] = value.astype(BF16)
            if ends:
                ends[k][q] = half_of(value, k).astype(BF16)


def advance(strip, sums, quarters, edge, with_ends):
    peers, pixels, _ = strip.shape
    step = 4
    specs = [pl.BlockSpec((step, edge, LANES), lambda i, k=k: (i, k, 0)) for k in quarters]
    whole = lambda n: pl.BlockSpec((step, n, LANES), lambda i: (i, 0, 0))
    sizes = [edge, edge] + ([edge // 2, edge // 2] if with_ends else [])
    return pl.pallas_call(
        advance_kernel,
        grid=(peers // step,),
        in_specs=[specs[0], specs[0], specs[1], specs[1]],
        out_specs=[whole(n) for n in sizes],
        out_shape=[pltpu.HBM((peers, n, LANES), BF16) for n in sizes],
        compiler_params=pltpu.CompilerParams(vmem_limit_bytes=63 * MIB),
        cost_estimate=cost(8 * peers * pixels * LANES, 3 * peers * pixels * LANES),
        name="advance_ends" if with_ends else "advance_middle",
    )(strip, sums, strip, sums)


def final_kernel(
    parts, mixed, obs, turned, out, misfit,
    held, code, made, rest, seen, spectra, come, came, go, went, side,
):
    blocks, block, atoms = held.shape
    step = block // STEPS
    wide = WIDE * step
    bands = rest.shape[2]
    reads, writes = [], []
    for i in range(STEPS):
        at = pl.ds(i * step, step)
        woven = pl.ds(i * step * blocks, step * blocks)
        reads.append(
            (
                pltpu.make_async_copy(parts.at[:, at, :], held.at[:, at, :], come.at[i]),
                pltpu.make_async_copy(mixed.at[:, woven, :], code.at[:, woven, :], came.at[i]),
            )
        )
        writes.append(pltpu.make_async_copy(made.at[:, at, :], out.at[:, at, :], go.at[i]))
    others = (
        pltpu.make_async_copy(turned, spectra, side.at[0]),
        pltpu.make_async_copy(obs, seen, side.at[1]),
    )
    for i, pair in enumerate(reads[:AHEAD]):
        for copy in pair:
            copy.start()
        if i == 0:
            for copy in others:
                copy.start()
    for i in range(STEPS):
        for copy in reads[i]:
            copy.wait()
        if i + AHEAD < STEPS:
            for copy in reads[i + AHEAD]:
                copy.start()
        at = slice(i * step, (i + 1) * step)
        woven = slice(i * step * blocks, (i + 1) * step * blocks)
        for p in range(mixed.shape[0]):
            lanes = slice(p * LANES, (p + 1) * LANES)
            sums = unweave(decode_positive(code[p, woven, :]))
            for j in range(blocks):
                value = halves(held[j, at, lanes]) + (1.0 / TOTAL) * sums[j]
                made[j, at, lanes] = jnp.maximum(value, 0.0).reshape(step, LANES).astype(BF16)
        writes[i].start()
        if i == 0:
            for copy in others:
                copy.wait()
        if (i + 1) % WIDE == 0:
            k = i // WIDE
            rows = pl.ds(k * wide, wide)
            rebuilt = jnp.dot(
                made[:, k * wide : (k + 1) * wide, :].reshape(blocks * wide, atoms),
                spectra[...],
                preferred_element_type=F32,
            )
            for j in range(blocks):
                real = seen[j, k * wide : (k + 1) * wide, :].astype(F32)
                less = real - rebuilt[j * wide : (j + 1) * wide]
                rest[j, k * wide : (k + 1) * wide, :] = less[:, :bands]
            writes.append(
                pltpu.make_async_copy(rest.at[:, rows, :], misfit.at[:, rows, :], went.at[k])
            )
            writes[-1].start()
    for copy in writes:
        copy.wait()


def final(parts, mixed, obs, turned, bands):
    peers, pixels, _ = mixed.shape
    atoms = parts.shape[2]
    obs = obs.reshape(BLOCKS, pixels // BLOCKS, obs.shape[1])
    hbm = pl.BlockSpec(memory_space=pltpu.HBM)
    left = (BLOCKS, pixels // BLOCKS, bands)
    return pl.pallas_call(
        final_kernel,
        in_specs=[hbm, hbm, hbm, hbm],
        out_specs=[hbm, hbm],
        out_shape=[pltpu.HBM(parts.shape, BF16), pltpu.HBM(left, F32)],
        scratch_shapes=[
            pltpu.VMEM(parts.shape, F32),
            pltpu.VMEM((peers, pixels, LANES), mixed.dtype),
            pltpu.VMEM(parts.shape, BF16),
            pltpu.VMEM(left, F32),
            pltpu.VMEM(obs.shape, obs.dtype),
            pltpu.VMEM(turned.shape, turned.dtype),
            pltpu.SemaphoreType.DMA((STEPS,)),
            pltpu.SemaphoreType.DMA((STEPS,)),
            pltpu.SemaphoreType.DMA((STEPS,)),
            pltpu.SemaphoreType.DMA((STEPS // WIDE,)),
            pltpu.SemaphoreType.DMA((2,)),
        ],
        compiler_params=pltpu.CompilerParams(vmem_limit_bytes=63 * MIB),
        cost_estimate=cost(2 * pixels * atoms * BANDS_PAD, 8 * pixels * atoms),
        name="final",
    )(parts, mixed, obs, turned)


def shifted(array, axis, up):
    peers = lax.axis_size(axis)
    pairs = [(k, k + 1) for k in range(peers - 1)]
    return lax.ppermute(array, axis, pairs if up else [(b, a) for a, b in pairs])


def exchanged(pieces):
    return lax.all_to_all(pieces, "col", 0, 0, tiled=True)


def strip_ends(strip, pixels, edge):
    def rows(a, h):
        tiles = a.reshape(a.shape[0], edge // 16, 2, 8, LANES)
        return tiles[:, :, h].reshape(a.shape[0], edge // 2, LANES)

    return rows(strip[:, :edge], 0), rows(strip[:, pixels - edge : pixels], 1)


def strip_halos(first, last):
    above = shifted(last, "row", True)
    below = shifted(first, "row", False)
    return above, below


def local(
    observed, library, warm, match_peer, match_slot, match_count, match_weight, wanted, threshold
):
    tile_rows, tile_cols, atoms = warm.shape
    bands = library.shape[0]
    pixels = tile_rows * tile_cols
    peers = lax.axis_size("col")
    flat = warm.reshape(pixels, atoms)

    pieces = spread(
        flat, BLOCKS, peers,
        match_peer, match_slot, match_count, match_weight, wanted,
    )
    strip = exchanged(pieces)
    lib = jnp.pad(library, ((0, BANDS_PAD - bands), (0, 0)))
    obs = jnp.pad(observed.reshape(pixels, bands), ((0, 0), (0, BANDS_PAD - bands)))
    inv = gram_inverse(lib)
    thr = threshold[None, :]

    by_block = flat.reshape(BLOCKS, pixels // BLOCKS, atoms)
    parts, primal, lifted = solve(True, tile_cols, obs, lib, inv, thr, (by_block,))
    strip_parts = exchanged(lifted)
    edge = BLOCKS * tile_cols
    above, below = strip_halos(*strip_ends(strip, pixels, edge))
    sums, weights = mix(encode_fixed, tile_cols, strip, above, below)
    mixed = exchanged(sums)
    first, last, *ends = advance(strip_parts, sums, (0, 3), edge, True)
    above, below = strip_halos(*ends)
    middle = advance(strip_parts, sums, (1, 2), edge, False)
    strip = (first, *middle, last)
    sums = mix(encode_positive, tile_cols, strip, above, below, weights)
    mixed_again = exchanged(sums)
    parts = solve(False, tile_cols, obs, lib, inv, thr, (parts, primal, mixed))
    abundance, misfit = final(parts, mixed_again, obs, lib.T, bands)
    return (
        abundance.reshape(tile_rows, tile_cols, atoms),
        misfit.reshape(tile_rows, tile_cols, bands),
    )


def solution(mesh):
    return jax.shard_map(
        local,
        mesh=mesh,
        in_specs=(
            P("row", "col", None),
            P(),
            P("row", "col", None),
            P("row", "col", None),
            P("row", "col", None),
            P("row", "col"),
            P("row", "col", None),
            P("row", "col", None),
            P(),
        ),
        out_specs=(P("row", "col", None), P("row", "col", None)),
        check_vma=False,
    )
```
